256 devices in a mesh: grp: 4 (over x), dev: 64 (over y, z, core).
Axes of the slice: x: 4, y: 4, z: 8, core: 2. Of those that a mesh axis runs over, the one named last changes fastest.
Arguments:
- obs_coord: float32 [3, 1048576], P(None, ('grp', 'dev')), may hold values from -1 to 1
- obs_resid: float32 [1048576], P(('grp', 'dev')), may hold values from -6 to 6
- obs_weight: float32 [1048576], P(('grp', 'dev')), may hold values from 0.5 to 2
- obs_dest: int32 [1048576], P(('grp', 'dev')), may hold values from 0 to 63, as said below
- obs_send_slot: int32 [1048576], P(('grp', 'dev')), may hold values from 0 to 127, as said below
- obs_elem: int32 [1048576], P(('grp', 'dev')), may hold values from 0 to 255, as said below
- obs_slot: int32 [1048576], P(('grp', 'dev')), may hold values from 0 to 31, as said below
Outputs:
- nodal: float32 [16, 512, 8, 512], P('grp', 'dev')
- total_cost: float32 [], replicated
The draws below stay inside these ranges and needn't reach their ends.
Inputs may be any that keep to these rules, and one draw needn't show every extreme that they name: `obs_dest`: from the rows of one device, at most 128 observations go to any one destination; in every group one destination receives exactly 128 from every device of the group. `obs_send_slot`: distinct among the rows of one device with the same obs_dest. `obs_elem`: together with obs_slot distinct among all observations of a group with the same obs_dest. `obs_slot`: on every destination some element uses all 32 slots.
All inputs are finite; a program needn't handle non-finite values.
Results may differ from the reference program's by a relative error of at most 0.00017.
Values sent between devices are 32-bit elements; how exact they have to be, the bound alone decides.
A program may use at most 64 MiB of HBM per device.

```python
import math
import jax
import jax.numpy as jnp
from jax import lax

OBS_DEV = 4096
EX = 4
EY = 8
EZ = 8
ELEM_DEV = 256
CAP = 128
SLOTS = 32
TOTAL_OBS = 1048576
NEX = 16
NEY = 512
N_GRP = 4
N_DEV = 64


def layout(key):
    peer_count = 2 * OBS_DEV // CAP
    group_count = TOTAL_OBS // (OBS_DEV * peer_count)
    cell_count = ELEM_DEV * SLOTS
    key_a, key_b, key_c, key_d, key_e = jax.random.split(key, 5)
    columns = jnp.arange(cell_count, dtype=jnp.int32)
    wanted = columns // CAP
    favored = jax.random.randint(key_a, (group_count, 1, 1), 0, peer_count, dtype=jnp.int32)
    jitter = jax.random.randint(key_b, (group_count, peer_count, cell_count), 1, 32768, dtype=jnp.int32)
    ranking = jnp.where(wanted[None, None, :] == favored, 0, jitter) * cell_count + columns
    picked = jnp.argsort(ranking, axis=-1)[:, :, :OBS_DEV].astype(jnp.int32)
    target = wanted[picked]
    row_ids = jnp.arange(OBS_DEV, dtype=jnp.int32)
    shuffle_keys = jax.random.randint(key_c, (group_count, peer_count, OBS_DEV), 0, 32768, dtype=jnp.int32) * OBS_DEV + row_ids
    mixing = jnp.argsort(shuffle_keys, axis=-1).astype(jnp.int32)
    target = jnp.take_along_axis(target, mixing, axis=-1)
    sorter = jnp.argsort(target, axis=-1, stable=True).astype(jnp.int32)
    sorted_target = jnp.take_along_axis(target, sorter, axis=-1)
    steps_row = jnp.broadcast_to(row_ids, sorted_target.shape)
    change = jnp.concatenate([jnp.ones((group_count, peer_count, 1), bool), sorted_target[:, :, 1:] != sorted_target[:, :, :-1]], axis=-1)
    starts = lax.cummax(jnp.where(change, steps_row, 0), axis=2)
    ranks_sorted = steps_row - starts
    inverse = jnp.argsort(sorter, axis=-1).astype(jnp.int32)
    send_slot = jnp.take_along_axis(ranks_sorted, inverse, axis=-1)
    owner = jnp.arange(group_count * peer_count, dtype=jnp.int32).reshape(group_count, peer_count, 1)
    segment = (owner * peer_count + target).reshape(-1)
    counts = jax.ops.segment_sum(jnp.ones_like(segment), segment, num_segments=group_count * peer_count * peer_count)
    counts = counts.reshape(group_count, peer_count, peer_count)
    earlier = jnp.cumsum(counts, axis=1) - counts
    arrival = jnp.take_along_axis(earlier, target, axis=2) + send_slot
    favored_elem = jax.random.randint(key_d, (group_count, peer_count, 1), 0, ELEM_DEV, dtype=jnp.int32)
    jitter_two = jax.random.randint(key_e, (group_count, peer_count, cell_count), 1, 32768, dtype=jnp.int32)
    ranking_two = jnp.where((columns // SLOTS)[None, None, :] == favored_elem, 0, jitter_two) * cell_count + columns
    table = jnp.argsort(ranking_two, axis=-1).astype(jnp.int32)
    group_ids = jnp.arange(group_count, dtype=jnp.int32).reshape(group_count, 1, 1)
    flat_index = ((group_ids * peer_count + target) * cell_count + arrival).reshape(-1)
    chosen = table.reshape(-1)[flat_index]
    return (target.reshape(-1).astype(jnp.int32), send_slot.reshape(-1).astype(jnp.int32), (chosen // SLOTS).astype(jnp.int32), (chosen % SLOTS).astype(jnp.int32))


def draw_obs_dest(key, part):
    return layout(jax.random.fold_in(key, 11))[0]


def draw_obs_send_slot(key, part):
    return layout(jax.random.fold_in(key, 11))[1]


def draw_obs_elem(key, part):
    return layout(jax.random.fold_in(key, 11))[2]


def draw_obs_slot(key, part):
    return layout(jax.random.fold_in(key, 11))[3]


def block_levels(stream_key, dims, pieces, smallest, top_value):
    level, own = 1.0, jax.random.fold_in(stream_key, 6)
    for dim, parts in pieces:
        draws = jnp.exp(jax.random.uniform(jax.random.fold_in(own, dim), (parts,), jnp.float32, smallest / len(pieces), top_value / len(pieces)))
        level = level * jnp.repeat(draws, dims[dim] // parts).reshape([-1 if axis == dim else 1 for axis in range(len(dims))])
    return level


def gaussian(stream_key, shape, width, reach, cuts=(), kind=jnp.bfloat16):
    loudness = block_levels(stream_key, shape, cuts, -0.22, 0.18) if cuts else 1.0
    array = jax.random.normal(stream_key, shape, jnp.float32) * width * loudness
    return jnp.minimum(jnp.maximum(array, -reach), reach).astype(kind)


def setup_inputs(seed: int = 0) -> dict:
    keys = jax.random.split(jax.random.key(seed), 8)
    obs_coord = jnp.clip(jax.random.uniform(keys[0], (3, TOTAL_OBS), jnp.float32, -1.0, 1.0) * block_levels(keys[0], (3, TOTAL_OBS), ((1, 256),), -0.4, 0.0), -1.0, 1.0)
    obs_resid = gaussian(keys[1], (TOTAL_OBS,), 1.0, 6.0, ((0, 256),), jnp.float32)
    obs_weight = jnp.clip(jnp.exp(math.log(2.0) - 1.3862944 * jax.random.uniform(keys[2], (TOTAL_OBS,), jnp.float32) ** block_levels(keys[2], (TOTAL_OBS,), ((0, 256),), -0.2, 0.2)), 0.5, 2.0)
    obs_dest = draw_obs_dest(jax.random.fold_in(keys[7], 71), 0)
    obs_send_slot = draw_obs_send_slot(jax.random.fold_in(keys[7], 71), 0)
    obs_elem = draw_obs_elem(jax.random.fold_in(keys[7], 71), 0)
    obs_slot = draw_obs_slot(jax.random.fold_in(keys[7], 71), 0)
    return {"obs_coord": obs_coord, "obs_resid": obs_resid, "obs_weight": obs_weight, "obs_dest": obs_dest, "obs_send_slot": obs_send_slot, "obs_elem": obs_elem, "obs_slot": obs_slot}


def basis_values(position):
    anchors = [-math.cos(math.pi * k / 7) for k in range(8)]
    basis = []
    for node_i in range(8):
        factor = jnp.ones_like(position)
        for node_m in range(8):
            if node_m != node_i:
                factor = factor * ((position - anchors[node_m]) / (anchors[node_i] - anchors[node_m]))
        basis.append(factor)
    return jnp.stack(basis)


def contract(first_w, second_w, third_w):
    outer = (first_w[:, None, :] * second_w[None, :, :]).reshape(64, ELEM_DEV, SLOTS)
    third = third_w.reshape(8, ELEM_DEV, SLOTS)
    mixed = jnp.einsum("aes,kes->eak", outer, third, precision=lax.Precision.HIGHEST)
    return mixed.reshape(ELEM_DEV, 512)


def combine(field, elem_dim, node_dim, from_low, from_high):
    count = field.shape[elem_dim]
    low_plane = lax.slice_in_dim(field, 0, 1, axis=node_dim)
    high_plane = lax.slice_in_dim(field, 7, 8, axis=node_dim)
    after = jnp.concatenate([lax.slice_in_dim(low_plane, 1, count, axis=elem_dim), from_high], axis=elem_dim)
    before = jnp.concatenate([from_low, lax.slice_in_dim(high_plane, 0, count - 1, axis=elem_dim)], axis=elem_dim)
    middle = lax.slice_in_dim(field, 1, 7, axis=node_dim)
    return jnp.concatenate([low_plane + before, middle, high_plane + after], axis=node_dim)


def block_nodes(block):
    first_w = basis_values(block[0]) * block[3]
    return contract(first_w, basis_values(block[1]), basis_values(block[2]))


def reference(obs_coord, obs_resid, obs_weight, obs_dest, obs_send_slot, obs_elem, obs_slot):
    forcing = obs_weight * obs_resid
    total_cost = 0.5 * jnp.sum(forcing * obs_resid)
    cell_count = ELEM_DEV * SLOTS
    device_count = N_GRP * N_DEV
    source = jnp.arange(TOTAL_OBS, dtype=jnp.int32) // OBS_DEV
    group_index = source // N_DEV
    device = group_index * N_DEV + obs_dest
    position = device * cell_count + obs_elem * SLOTS + obs_slot
    values = jnp.concatenate([obs_coord, forcing[None, :]], axis=0)
    packed = jnp.zeros((4, device_count * cell_count), obs_coord.dtype).at[:, position].set(values)
    blocks = packed.reshape(4, device_count, cell_count).transpose(1, 0, 2)
    raw = lax.map(block_nodes, blocks)
    raw = raw.reshape(N_GRP, N_DEV, EX, EY, EZ, 512).transpose(0, 2, 1, 3, 4, 5)
    field = raw.reshape(NEX, NEY, EZ, 8, 8, 8)
    for elem_dim in range(3):
        node_dim = elem_dim + 3
        edge = lax.slice_in_dim(lax.slice_in_dim(field, 0, 1, axis=node_dim), 0, 1, axis=elem_dim)
        empty = jnp.zeros_like(edge)
        field = combine(field, elem_dim, node_dim, empty, empty)
    return field.reshape(NEX, NEY, EZ, 512), total_cost
```

```python
import functools
import math

import jax
import jax.numpy as jnp
from jax import lax
from jax.experimental import pallas as pl
from jax.experimental.pallas import tpu as pltpu
from jax.sharding import PartitionSpec as P

CAP = 128
ELEM = 256
NODES = 512
COPLANE = 16
NODE_POINTS = [-math.cos(math.pi * k / 7) for k in range(8)]
NODE_SCALE = [
    1.0 / math.prod(NODE_POINTS[a] - NODE_POINTS[m] for m in range(8) if m != a)
    for a in range(8)
]
NT = (((1,), (1,)), ((), ()))


def peer_order(n_dev):
    def hops(offset):
        y, z = offset // COPLANE, (offset % COPLANE) // 2
        return min(y, max(n_dev // COPLANE, 1) - y) + min(z, COPLANE // 2 - z)

    return [0] + sorted(range(1, n_dev), key=lambda o: (hops(o), o))


def lanes_of(shape):
    return lax.broadcasted_iota(jnp.int32, shape, len(shape) - 1)


def rows_of(shape):
    return lax.broadcasted_iota(jnp.int32, shape, len(shape) - 2)


def split(value):
    high = value.astype(jnp.bfloat16).astype(jnp.float32)
    return high, value - high


def basis(t):
    shape = (8, t.shape[1])
    t = jnp.broadcast_to(t, shape)
    row = rows_of(shape)
    out = None
    for m in range(8):
        factor = jnp.where(row == m, jnp.float32(NODE_SCALE[m]), t - jnp.float32(NODE_POINTS[m]))
        out = factor if out is None else out * factor
    return out


def kernel(
    n_grp, n_dev, coord, resid, weight, dest, slot, elem, out, cost,
    coord_v, resid_v, weight_v, dest_v, slot_v, elem_v,
    lhs, pick, send, recv, xa, xb, oha, ohb, acc, fin,
    c1s, c1r, c2s, c2r, halo_g, halo_d, halo_c, dsend,
    in_sem, send_sem, recv_sem, c1_ssem, c1_rsem, c2_ssem, c2_rsem, h_ssem, h_rsem,
):
    g, d = lax.axis_index("grp"), lax.axis_index("dev")
    co = min(COPLANE, n_dev)
    planes = n_dev // co
    order = peer_order(n_dev)
    here = lax.rem(d, co)
    block = d - here

    def at(dg, dd):
        return {"grp": lax.rem(g + dg + n_grp, n_grp), "dev": lax.rem(d + dd + n_dev, n_dev)}

    barrier = pltpu.get_barrier_semaphore()
    corners = [(-1, -1), (-1, 1), (1, -1), (1, 1)]
    peers = [(0, o) for o in order[1:]]
    peers += [(k, p * co) for k in range(1, n_grp) for p in range(planes)]
    peers += corners
    for dg, dd in peers:
        pl.semaphore_signal(barrier, inc=1, device_id=at(dg, dd))

    loads = [
        pltpu.make_async_copy(src, dst, in_sem.at[i])
        for i, (src, dst) in enumerate(
            [(dest, dest_v), (slot, slot_v), (elem, elem_v), (coord, coord_v), (resid, resid_v), (weight, weight_v)]
        )
    ]
    for load in loads:
        load.start()
    for load in loads:
        load.wait()

    def fill(j, carry):
        def pair(ref):
            return jnp.concatenate([ref[pl.ds(2 * j, 1), :], ref[pl.ds(2 * j + 1, 1), :]], axis=1)

        cols = pl.ds(pl.multiple_of(j * 256, 256), 256)
        here_mask = rows_of((n_dev, 256)) == pair(dest_v)
        vals = [coord_v[c : c + 1, cols] for c in range(3)]
        vals.append(pair(weight_v) * pair(resid_v))
        for c, value in enumerate(vals):
            for h, part in enumerate(split(value)):
                row = (2 * c + h) * n_dev
                lhs[row : row + n_dev, cols] = jnp.where(here_mask, part, 0.0).astype(jnp.bfloat16)
        ids = pair(elem_v).astype(jnp.float32)
        lhs[8 * n_dev : 9 * n_dev, cols] = jnp.where(here_mask, ids, 0.0).astype(jnp.bfloat16)
        slot_mask = rows_of((CAP, 256)) == pair(slot_v)
        pick[:, cols] = jnp.where(slot_mask, 1.0, 0.0).astype(jnp.bfloat16)
        return carry

    lax.fori_loop(0, resid_v.shape[0] // 2, fill, 0)
    packed = lax.dot_general(lhs[...], pick[...], NT, preferred_element_type=jnp.float32)
    part = [packed[k * n_dev : (k + 1) * n_dev] for k in range(9)]
    for c in range(4):
        send[:, c, :] = part[2 * c] + part[2 * c + 1]
    send[:, 4, :] = part[8]
    r = resid_v[...]
    c1s[...] = jnp.sum(weight_v[...] * r * r, axis=0, keepdims=True)

    recv[0] = send[d]
    c1r[here] = c1s[...]

    pl.semaphore_wait(barrier, len(peers))

    def message(k):
        return pltpu.make_async_remote_copy(
            src_ref=send.at[lax.rem(d + order[k], n_dev)],
            dst_ref=recv.at[k],
            send_sem=send_sem.at[k],
            recv_sem=recv_sem.at[k],
            device_id=at(0, order[k]),
        )

    messages = [message(k) for k in range(1, n_dev)]
    for m in reversed(messages):
        m.start()

    def partial_one(k):
        return pltpu.make_async_remote_copy(
            src_ref=c1s, dst_ref=c1r.at[here], send_sem=c1_ssem.at[k], recv_sem=c1_rsem.at[k],
            device_id={"grp": g, "dev": block + lax.rem(here + k, co)},
        )

    ones = [partial_one(k) for k in range(1, co)]
    for m in ones:
        m.start()

    acc[...] = jnp.zeros_like(acc)
    xb[...] = jnp.zeros_like(xb)
    ohb[...] = jnp.zeros_like(ohb)

    def build(p, x, oh):
        first, second = recv[2 * p], recv[2 * p + 1]

        def row(c):
            return jnp.concatenate([first[c : c + 1], second[c : c + 1]], axis=1)

        fa = basis(row(0)) * row(3)
        fb = basis(row(1))
        fc = basis(row(2))
        for a in range(8):
            ab = fa[a : a + 1] * fb
            for b in range(0, 8, 2):
                full = jnp.concatenate([ab[b : b + 1] * fc, ab[b + 1 : b + 2] * fc], axis=0)
                high = full.astype(jnp.bfloat16)
                low = (full - high.astype(jnp.float32)).astype(jnp.bfloat16)
                at_row = (8 * a + b) * 8
                x[at_row : at_row + 16, 0:256] = high
                x[at_row : at_row + 16, 256:512] = low
        ids = row(4).astype(jnp.int32)
        oh[...] = jnp.where(rows_of((ELEM, 256)) == ids, 1.0, 0.0).astype(jnp.bfloat16)

    def product(x, oh):
        return lax.dot_general(
            x[:, 0:256], oh[...], NT, preferred_element_type=jnp.float32
        ) + lax.dot_general(x[:, 256:512], oh[...], NT, preferred_element_type=jnp.float32)

    def arrived(k):
        pltpu.make_async_remote_copy(
            src_ref=send.at[0], dst_ref=recv.at[k], send_sem=send_sem.at[k], recv_sem=recv_sem.at[k],
            device_id=at(0, 1),
        ).wait_recv()

    def two_pairs(t):
        acc[...] += product(xb, ohb)
        build(2 * t, xa, oha)
        acc[...] += product(xa, oha)
        build(2 * t + 1, xb, ohb)

    for k in range(1, 4):
        arrived(k)
    two_pairs(0)

    def body(t, carry):
        for k in range(4):
            arrived(4 * t + k)
        two_pairs(t)
        return carry

    if n_dev > 4:
        lax.fori_loop(1, n_dev // 4, body, 0)
    acc[...] += product(xb, ohb)

    lane = lanes_of((8, ELEM))

    def rg(ref, a, b):
        return ref[(8 * a + b) * 8 : (8 * a + b) * 8 + 8, :]

    def put(ref, a, b, value):
        ref[(8 * a + b) * 8 : (8 * a + b) * 8 + 8, :] = value

    def move(x, k):
        return pltpu.roll(x, k % x.shape[1], 1)

    for b in range(8):
        low, high = rg(acc, 0, b), rg(acc, 7, b)
        put(acc, 0, b, low + jnp.where(lane >= 64, move(high, 64), 0.0))
        put(acc, 7, b, high + jnp.where(lane < 192, move(low, -64), 0.0))
    half = lanes_of((8, 128))
    for a in range(8):
        for side, b in ((0, 0), (1, 7)):
            x = rg(acc, a, b)
            near = ((half >> 3) & 7) == b
            left = jnp.where(near, x[:, :128], 0.0)
            right = jnp.where(near, x[:, 128:], 0.0)
            dsend[side, 8 * a : 8 * a + 8, :] = left + move(right, 8 if b == 0 else -8)

    for k in range(1, co):
        pltpu.make_async_remote_copy(
            src_ref=c1s, dst_ref=c1r.at[here], send_sem=c1_ssem.at[k], recv_sem=c1_rsem.at[k],
            device_id=at(0, 1),
        ).wait_recv()
    total = c1r[0]
    for k in range(1, co):
        total += c1r[k]
    c2s[...] = total
    mine = g * planes + block // co
    c2r[mine] = total

    def halo(i, src, dst, dg, dd):
        return pltpu.make_async_remote_copy(
            src_ref=src, dst_ref=dst, send_sem=h_ssem.at[i], recv_sem=h_rsem.at[i],
            device_id=at(dg, dd),
        )

    halos = [
        halo(0, acc.at[0:64, 0:128], halo_g.at[0], -1, 0),
        halo(1, acc.at[448:512, 128:256], halo_g.at[1], 1, 0),
        halo(2, dsend.at[0], halo_d.at[0], 0, -1),
        halo(3, dsend.at[1], halo_d.at[1], 0, 1),
        halo(4, acc.at[0:8, 0:128], halo_c.at[0], -1, -1),
        halo(5, acc.at[56:64, 0:128], halo_c.at[1], -1, 1),
        halo(6, acc.at[448:456, 128:256], halo_c.at[2], 1, -1),
        halo(7, acc.at[504:512, 128:256], halo_c.at[3], 1, 1),
    ]
    for m in halos:
        m.start()
    rest = [(k, p) for k in range(n_grp) for p in range(planes) if k or p]
    twos = [
        pltpu.make_async_remote_copy(
            src_ref=c2s, dst_ref=c2r.at[mine], send_sem=c2_ssem.at[i], recv_sem=c2_rsem.at[i],
            device_id=at(k, p * co),
        )
        for i, (k, p) in enumerate(rest)
    ]
    for m in twos:
        m.start()
    for m in halos:
        m.wait_recv()

    up_g, down_g = g > 0, g < n_grp - 1
    up_d, down_d = d > 0, d < n_dev - 1
    ey = (lane >> 3) & 7
    ez = lane & 7

    def wide(x):
        return jnp.concatenate([x, x], axis=1)

    for b in range(8):
        from_low = move(halo_g[1, 8 * b : 8 * b + 8, :], 64)
        from_high = move(halo_g[0, 8 * b : 8 * b + 8, :], 64)
        put(fin, 0, b, rg(acc, 0, b) + jnp.where((lane < 64) & up_g, wide(from_low), 0.0))
        put(fin, 7, b, rg(acc, 7, b) + jnp.where((lane >= 192) & down_g, wide(from_high), 0.0))
    for a in range(1, 7):
        fin[64 * a : 64 * a + 64, :] = acc[64 * a : 64 * a + 64, :]
    for a in range(8):
        low, high = rg(fin, a, 0), rg(fin, a, 7)
        theirs = halo_d[1, 8 * a : 8 * a + 8, :]
        to_low = jnp.concatenate([move(theirs, -56), move(theirs, -48)], axis=1)
        theirs = halo_d[0, 8 * a : 8 * a + 8, :]
        to_high = jnp.concatenate([move(theirs, 56), move(theirs, 48)], axis=1)
        if a == 0:
            to_low += jnp.where((lane < 8) & up_g, wide(move(halo_c[3], -120)), 0.0)
            to_high += jnp.where((lane >= 56) & (lane < 64) & up_g, wide(move(halo_c[2], -8)), 0.0)
        if a == 7:
            to_low += jnp.where((lane >= 192) & (lane < 200) & down_g, wide(move(halo_c[1], 8)), 0.0)
            to_high += jnp.where((lane >= 248) & down_g, wide(move(halo_c[0], 120)), 0.0)
        new_low = jnp.where(ey > 0, move(high, 8), jnp.where(up_d, to_low, 0.0))
        new_high = jnp.where(ey < 7, move(low, -8), jnp.where(down_d, to_high, 0.0))
        put(fin, a, 0, low + new_low)
        put(fin, a, 7, high + new_high)
    row = rows_of((8, ELEM))
    for a in range(8):
        for b in range(8):
            x = rg(fin, a, b)
            z = jnp.where(row == 7, move(x, 1), move(x, -1))
            to_low = jnp.where((row == 0) & (ez > 0), pltpu.roll(z, 1, 0), 0.0)
            to_high = jnp.where((row == 7) & (ez < 7), pltpu.roll(z, 7, 0), 0.0)
            put(fin, a, b, x + to_low + to_high)
    out[...] = fin[...].T

    for m in twos:
        m.wait_recv()
    total = c2r[0]
    for k in range(1, n_grp * planes):
        total += c2r[k]
    cost[0, 0] = 0.5 * jnp.sum(total)
    for m in messages + ones + halos + twos:
        m.wait_send()


def on_device(coord, resid, weight, dest, slot, elem, n_grp, n_dev):
    rows = resid.shape[0] // 128
    flat = [x.reshape(rows, 128) for x in (resid, weight, dest, slot, elem)]
    co = min(COPLANE, n_dev)
    blocks = n_grp * (n_dev // co)
    f32, bf16, i32 = jnp.float32, jnp.bfloat16, jnp.int32
    dma = pltpu.SemaphoreType.DMA
    out, cost = pl.pallas_call(
        functools.partial(kernel, n_grp, n_dev),
        out_shape=(
            jax.ShapeDtypeStruct((ELEM, NODES), f32),
            jax.ShapeDtypeStruct((1, 1), f32),
        ),
        in_specs=[pl.BlockSpec(memory_space=pl.ANY)] * 6,
        out_specs=(
            pl.BlockSpec(memory_space=pltpu.VMEM),
            pl.BlockSpec(memory_space=pltpu.SMEM),
        ),
        scratch_shapes=[
            pltpu.VMEM(coord.shape, f32),
            pltpu.VMEM((rows, 128), f32),
            pltpu.VMEM((rows, 128), f32),
            pltpu.VMEM((rows, 128), i32),
            pltpu.VMEM((rows, 128), i32),
            pltpu.VMEM((rows, 128), i32),
            pltpu.VMEM((9 * n_dev, rows * 128), bf16),
            pltpu.VMEM((CAP, rows * 128), bf16),
            pltpu.VMEM((n_dev, 5, CAP), f32),
            pltpu.VMEM((n_dev, 5, CAP), f32),
            pltpu.VMEM((NODES, 512), bf16),
            pltpu.VMEM((NODES, 512), bf16),
            pltpu.VMEM((ELEM, 256), bf16),
            pltpu.VMEM((ELEM, 256), bf16),
            pltpu.VMEM((NODES, ELEM), f32),
            pltpu.VMEM((NODES, ELEM), f32),
            pltpu.VMEM((1, 128), f32),
            pltpu.VMEM((co, 1, 128), f32),
            pltpu.VMEM((1, 128), f32),
            pltpu.VMEM((blocks, 1, 128), f32),
            pltpu.VMEM((2, 64, 128), f32),
            pltpu.VMEM((2, 64, 128), f32),
            pltpu.VMEM((4, 8, 128), f32),
            pltpu.VMEM((2, 64, 128), f32),
            dma((6,)),
            dma((n_dev,)),
            dma((n_dev,)),
            dma((co,)),
            dma((co,)),
            dma((blocks,)),
            dma((blocks,)),
            dma((8,)),
            dma((8,)),
        ],
        compiler_params=pltpu.CompilerParams(collective_id=0, has_side_effects=True),
    )(coord, *flat)
    return out.reshape(4, 8, 8, NODES), cost.reshape(())


def solution(mesh):
    n_grp, n_dev = mesh.shape["grp"], mesh.shape["dev"]
    rows = P(("grp", "dev"))

    def step(obs_coord, obs_resid, obs_weight, obs_dest, obs_send_slot, obs_elem, obs_slot):
        del obs_slot
        return on_device(
            obs_coord, obs_resid, obs_weight, obs_dest, obs_send_slot, obs_elem, n_grp, n_dev
        )

    return jax.shard_map(
        step,
        mesh=mesh,
        in_specs=(P(None, ("grp", "dev")), rows, rows, rows, rows, rows, rows),
        out_specs=(P("grp", "dev", None, None), P()),
        check_vma=False,
    )
```

```python
import functools
import math

import jax
import jax.numpy as jnp
from jax import lax
from jax.experimental import pallas as pl
from jax.experimental.pallas import tpu as pltpu
from jax.sharding import PartitionSpec as P

CAP = 128
ELEM = 256
NODES = 512
COPLANE = 16
PEERS = 64
NODE_POINTS = [-math.cos(math.pi * k / 7) for k in range(8)]
NODE_SCALE = [
    1.0 / math.prod(NODE_POINTS[a] - NODE_POINTS[m] for m in range(8) if m != a)
    for a in range(8)
]
NT = (((1,), (1,)), ((), ()))
F32, BF16, I32 = jnp.float32, jnp.bfloat16, jnp.int32
EDGE = (0, 7)
OUTER = [(a, b) for a in range(8) for b in range(8) if a in EDGE or b in EDGE]
INNER = [(a, b) for a in range(8) for b in range(8) if not (a in EDGE or b in EDGE)]
OUTER.sort(key=lambda ab: (EDGE.index(ab[0]) if ab[0] in EDGE else 2, ab))
GROUPS = OUTER + INNER
PLACE = {ab: 8 * i for i, ab in enumerate(GROUPS)}
SPLIT = 8 * len(OUTER)


def peer_order(n_dev):
    def hops(offset):
        y, z = offset // COPLANE, (offset % COPLANE) // 2
        return min(y, max(n_dev // COPLANE, 1) - y) + min(z, COPLANE // 2 - z)

    return [0] + sorted(range(1, n_dev), key=lambda o: (hops(o), o))


def lanes_of(shape):
    return lax.broadcasted_iota(I32, shape, len(shape) - 1)


def rows_of(shape):
    return lax.broadcasted_iota(I32, shape, len(shape) - 2)


def high_of(value):
    return value.astype(BF16).astype(F32)


def one_hot(ids, count):
    shape = (count, ids.shape[1])
    ids = jnp.broadcast_to(ids, (16, ids.shape[1])).astype(BF16)
    ids = jnp.concatenate([ids] * (count // 16), axis=0)
    row = rows_of(shape).astype(F32).astype(BF16)
    return jnp.where(row == ids, jnp.ones(shape, BF16), jnp.zeros(shape, BF16))


def basis(t):
    shape = (8, t.shape[1])
    t = jnp.broadcast_to(t, shape)
    row = rows_of(shape)
    out = None
    for m in range(8):
        factor = jnp.where(row == m, F32(NODE_SCALE[m]), t - F32(NODE_POINTS[m]))
        out = factor if out is None else out * factor
    return out


def move(x, k):
    return pltpu.roll(x, k % x.shape[1], 1)


def exchange_kernel(
    n_grp, n_dev, coord, resid, weight, dest, slot, elem, mid, cost,
    coord_v, resid_v, weight_v, dest_v, slot_v, elem_v,
    lhs, pick, send, recv, xo, xi, oh, acc, outer,
    c1s, c1r, c2s, c2r, halo_g, halo_d, halo_c, dsend,
    in_sem, send_sem, recv_sem, c1_ssem, c1_rsem, c2_ssem, c2_rsem, h_ssem, h_rsem,
):
    g, d = lax.axis_index("grp"), lax.axis_index("dev")
    co = min(COPLANE, n_dev)
    planes = n_dev // co
    order = peer_order(n_dev)
    here = lax.rem(d, co)
    block = d - here

    def at(dg, dd):
        return {"grp": lax.rem(g + dg + n_grp, n_grp), "dev": lax.rem(d + dd + n_dev, n_dev)}

    loads = [
        pltpu.make_async_copy(src, dst, in_sem.at[i])
        for i, (src, dst) in enumerate(
            [(dest, dest_v), (slot, slot_v), (elem, elem_v), (coord, coord_v), (resid, resid_v), (weight, weight_v)]
        )
    ]
    for load in loads:
        load.start()

    barrier = pltpu.get_barrier_semaphore()
    corners = [(-1, -1), (-1, 1), (1, -1), (1, 1)]
    peers = [(k, p * co) for k in range(1, n_grp) for p in range(planes)]
    peers += corners
    peers += [(0, o) for o in order[1:]]
    for dg, dd in reversed(peers):
        pl.semaphore_signal(barrier, inc=1, device_id=at(dg, dd))
    for load in loads:
        load.wait()

    for j in range(resid_v.shape[0] // 2):
        def pair(ref):
            return jnp.concatenate([ref[2 * j : 2 * j + 1, :], ref[2 * j + 1 : 2 * j + 2, :]], axis=1)

        cols = slice(256 * j, 256 * j + 256)
        to = pair(dest_v)
        upper = to >> 5
        mask = one_hot((to - 32 * upper).astype(F32), 32)
        pick[:, cols] = one_hot((upper * CAP + pair(slot_v)).astype(F32), 256)
        parts = []
        for value in [coord_v[c : c + 1, cols] for c in range(3)] + [pair(weight_v) * pair(resid_v)]:
            high = high_of(value)
            parts += [high, value - high]
        parts.append(pair(elem_v).astype(F32))
        for i, part in enumerate(parts):
            wide = jnp.broadcast_to(part, (16, 256)).astype(BF16)
            lhs[32 * i : 32 * i + 32, cols] = mask * jnp.concatenate([wide, wide], axis=0)
    packed = lax.dot_general(lhs[...], pick[...], NT, preferred_element_type=F32)
    part = [packed[32 * k : 32 * k + 32] for k in range(9)]
    values = [part[2 * c] + part[2 * c + 1] for c in range(4)] + [part[8]]
    for c, value in enumerate(values):
        send[0:32, c, :] = value[:, :CAP]
        send[32:64, c, :] = value[:, CAP:]
    r = resid_v[...]
    c1s[...] = jnp.sum(weight_v[...] * r * r, axis=0, keepdims=True)

    recv[0] = send[d]
    c1r[here] = c1s[...]

    pl.semaphore_wait(barrier, len(peers))

    bounds = [0, 24, 44, 56, 64] if n_dev == 64 else [0, 2, 4]
    chunks = list(zip(bounds[:-1], bounds[1:]))
    chunk_of = [i for i, (first, last) in enumerate(chunks) for _ in range(first, last)]

    def message(k):
        to = lax.rem(d + order[k], n_dev)
        return pltpu.make_async_remote_copy(
            src_ref=send.at[to],
            dst_ref=recv.at[k],
            send_sem=send_sem,
            recv_sem=recv_sem.at[chunk_of[k]],
            device_id={"grp": g, "dev": to},
        )

    def await_bytes(ref, sem):
        pltpu.make_async_copy(ref, ref, sem).wait()

    for k in range(1, n_dev):
        message(k).start()

    def partial_one(k):
        return pltpu.make_async_remote_copy(
            src_ref=c1s, dst_ref=c1r.at[here], send_sem=c1_ssem, recv_sem=c1_rsem,
            device_id={"grp": g, "dev": block + lax.rem(here + k, co)},
        )

    for k in range(1, co):
        partial_one(k).start()

    mine = g * planes + block // co
    rest = [(k, p) for k in range(n_grp) for p in range(planes) if k or p]
    twos = [
        pltpu.make_async_remote_copy(
            src_ref=c2s, dst_ref=c2r.at[mine], send_sem=c2_ssem, recv_sem=c2_rsem,
            device_id=at(k, p * co),
        )
        for k, p in rest
    ]

    def build(p):
        first, second = recv[2 * p], recv[2 * p + 1]

        def row(c):
            return jnp.concatenate([first[c : c + 1], second[c : c + 1]], axis=1)

        cols = slice(256 * p, 256 * p + 256)
        fa = basis(row(0)) * row(3)
        fb = basis(row(1))
        fc = basis(row(2))
        for i in range(0, 64, 2):
            full = jnp.concatenate(
                [fa[a : a + 1] * fb[b : b + 1] * fc for a, b in GROUPS[i : i + 2]], axis=0
            )
            high = full.astype(BF16)
            low = (full - high.astype(F32)).astype(BF16)
            ref, row_of, count = (xo, 8 * i, SPLIT) if 8 * i < SPLIT else (xi, 8 * i - SPLIT, NODES - SPLIT)
            ref[row_of : row_of + 16, cols] = high
            ref[count + row_of : count + row_of + 16, cols] = low
        oh[:, cols] = one_hot(row(4), ELEM)

    def product(ref, cols):
        return lax.dot_general(ref[:, cols], oh[:, cols], NT, preferred_element_type=F32)

    def arrived(i):
        first, last = max(chunks[i][0], 1), chunks[i][1]
        await_bytes(recv.at[first:last], recv_sem.at[i])

    def cols_of(first, last):
        return slice(128 * first, 128 * last)

    arrived(0)
    for p in range(chunks[0][0] // 2, chunks[0][1] // 2):
        build(p)
    for i, chunk in enumerate(chunks):
        if i + 1 < len(chunks):
            arrived(i + 1)
        now = product(xo, cols_of(*chunk))
        if i > 0:
            now = acc[...] + now
        if i + 1 < len(chunks):
            acc[...] = now
            for p in range(chunks[i + 1][0] // 2, chunks[i + 1][1] // 2):
                build(p)
        else:
            outer[...] = now[:SPLIT] + now[SPLIT:]
        if i == 1:
            await_bytes(c1r.at[1:co], c1_rsem)
            total = c1r[0]
            for k in range(1, co):
                total += c1r[k]
            c2s[...] = total
            c2r[mine] = total
            for m in twos:
                m.start()

    lane = lanes_of((8, ELEM))

    def rg(ref, a, b):
        return ref[PLACE[a, b] : PLACE[a, b] + 8, :]

    def put(ref, a, b, value):
        ref[PLACE[a, b] : PLACE[a, b] + 8, :] = value

    for b in range(8):
        low, high = rg(outer, 0, b), rg(outer, 7, b)
        put(outer, 0, b, low + jnp.where(lane >= 64, move(high, 64), 0.0))
        put(outer, 7, b, high + jnp.where(lane < 192, move(low, -64), 0.0))
    half = lanes_of((8, 128))
    for a in range(8):
        for side, b in ((0, 0), (1, 7)):
            plane = rg(outer, a, b)
            near = ((half >> 3) & 7) == b
            left = jnp.where(near, plane[:, :128], 0.0)
            right = jnp.where(near, plane[:, 128:], 0.0)
            dsend[side, 8 * a : 8 * a + 8, :] = left + move(right, 8 if b == 0 else -8)

    def halo(kind, src, dst, dg, dd):
        return pltpu.make_async_remote_copy(
            src_ref=src, dst_ref=dst, send_sem=h_ssem.at[kind], recv_sem=h_rsem.at[kind],
            device_id=at(dg, dd),
        )

    def tile(a, b, count, right):
        first = PLACE[a, b]
        return outer.at[first : first + 8 * count, (128 if right else 0) : (256 if right else 128)]

    halos = [
        halo(0, tile(0, 0, 8, False), halo_g.at[0], -1, 0),
        halo(0, tile(7, 0, 8, True), halo_g.at[1], 1, 0),
        halo(1, dsend.at[0], halo_d.at[0], 0, -1),
        halo(1, dsend.at[1], halo_d.at[1], 0, 1),
        halo(2, tile(0, 0, 1, False), halo_c.at[0], -1, -1),
        halo(2, tile(0, 7, 1, False), halo_c.at[1], -1, 1),
        halo(2, tile(7, 0, 1, True), halo_c.at[2], 1, -1),
        halo(2, tile(7, 7, 1, True), halo_c.at[3], 1, 1),
    ]
    for m in halos:
        m.start()
    left = product(xi, slice(0, n_dev * CAP))
    mid[SPLIT:, :] = left[: NODES - SPLIT] + left[NODES - SPLIT :]

    for kind, ref in enumerate((halo_g, halo_d, halo_c)):
        await_bytes(ref, h_rsem.at[kind])

    up_g, down_g = g > 0, g < n_grp - 1
    up_d, down_d = d > 0, d < n_dev - 1
    ey = (lane >> 3) & 7

    def wide(value):
        return jnp.concatenate([value, value], axis=1)

    planes_now = {ab: rg(outer, *ab) for ab in OUTER}
    for b in range(8):
        from_low = move(halo_g[1, 8 * b : 8 * b + 8, :], 64)
        from_high = move(halo_g[0, 8 * b : 8 * b + 8, :], 64)
        planes_now[0, b] += jnp.where((lane < 64) & up_g, wide(from_low), 0.0)
        planes_now[7, b] += jnp.where((lane >= 192) & down_g, wide(from_high), 0.0)
    for a in range(8):
        low, high = planes_now[a, 0], planes_now[a, 7]
        theirs = halo_d[1, 8 * a : 8 * a + 8, :]
        to_low = jnp.concatenate([move(theirs, -56), move(theirs, -48)], axis=1)
        theirs = halo_d[0, 8 * a : 8 * a + 8, :]
        to_high = jnp.concatenate([move(theirs, 56), move(theirs, 48)], axis=1)
        if a == 0:
            to_low += jnp.where((lane < 8) & up_g, wide(move(halo_c[3], -120)), 0.0)
            to_high += jnp.where((lane >= 56) & (lane < 64) & up_g, wide(move(halo_c[2], -8)), 0.0)
        if a == 7:
            to_low += jnp.where((lane >= 192) & (lane < 200) & down_g, wide(move(halo_c[1], 8)), 0.0)
            to_high += jnp.where((lane >= 248) & down_g, wide(move(halo_c[0], 120)), 0.0)
        new_low = jnp.where(ey > 0, move(high, 8), jnp.where(up_d, to_low, 0.0))
        new_high = jnp.where(ey < 7, move(low, -8), jnp.where(down_d, to_high, 0.0))
        planes_now[a, 0] = low + new_low
        planes_now[a, 7] = high + new_high
    for ab in OUTER:
        put(mid, *ab, planes_now[ab])

    await_bytes(c2r.at[1:], c2_rsem)
    total = c2r[0]
    for k in range(1, n_grp * planes):
        total += c2r[k]
    cost[...] = total
    await_bytes(recv.at[1:], send_sem)
    await_bytes(c1r.at[1:], c1_ssem)
    await_bytes(c2r.at[1:], c2_ssem)
    for kind, ref in enumerate((halo_g, halo_d, halo_c)):
        await_bytes(ref, h_ssem.at[kind])


def finish_kernel(mid, cost_row, out, cost):
    shape = (8, 128)
    ez = lanes_of(shape) & 7
    row = rows_of(shape)
    done = {}
    for ab in GROUPS:
        now = mid[PLACE[ab] : PLACE[ab] + 8, :]
        z = jnp.where(row == 7, move(now, 1), move(now, -1))
        to_low = jnp.where((row == 0) & (ez > 0), pltpu.roll(z, 1, 0), 0.0)
        to_high = jnp.where((row == 7) & (ez < 7), pltpu.roll(z, 7, 0), 0.0)
        done[ab] = now + to_low + to_high
    for a in range(0, 8, 2):
        both = jnp.concatenate([done[k, b] for k in (a, a + 1) for b in range(8)], axis=0)
        out[:, 64 * a : 64 * a + 128] = both.T
    cost[0, 0] = 0.5 * jnp.sum(cost_row[...])


def on_device(coord, resid, weight, dest, slot, elem, n_grp, n_dev):
    rows = resid.shape[0] // 128
    flat = [v.reshape(rows, 128) for v in (resid, weight, dest, slot, elem)]
    co = min(COPLANE, n_dev)
    blocks = n_grp * (n_dev // co)
    dma = pltpu.SemaphoreType.DMA
    vmem = pl.BlockSpec(memory_space=pltpu.VMEM)
    mid, cost_row = pl.pallas_call(
        functools.partial(exchange_kernel, n_grp, n_dev),
        out_shape=(
            jax.ShapeDtypeStruct((NODES, ELEM), F32),
            jax.ShapeDtypeStruct((1, 128), F32),
        ),
        in_specs=[pl.BlockSpec(memory_space=pltpu.HBM)] * 6,
        out_specs=(vmem, vmem),
        scratch_shapes=[
            pltpu.VMEM(coord.shape, F32),
            pltpu.VMEM((rows, 128), F32),
            pltpu.VMEM((rows, 128), F32),
            pltpu.VMEM((rows, 128), I32),
            pltpu.VMEM((rows, 128), I32),
            pltpu.VMEM((rows, 128), I32),
            pltpu.VMEM((9 * 32, rows * 128), BF16),
            pltpu.VMEM((256, rows * 128), BF16),
            pltpu.VMEM((PEERS, 5, CAP), F32),
            pltpu.VMEM((n_dev, 5, CAP), F32),
            pltpu.VMEM((2 * SPLIT, n_dev * CAP), BF16),
            pltpu.VMEM((2 * (NODES - SPLIT), n_dev * CAP), BF16),
            pltpu.VMEM((ELEM, n_dev * CAP), BF16),
            pltpu.VMEM((2 * SPLIT, ELEM), F32),
            pltpu.VMEM((SPLIT, ELEM), F32),
            pltpu.VMEM((1, 128), F32),
            pltpu.VMEM((co, 1, 128), F32),
            pltpu.VMEM((1, 128), F32),
            pltpu.VMEM((blocks, 1, 128), F32),
            pltpu.VMEM((2, 64, 128), F32),
            pltpu.VMEM((2, 64, 128), F32),
            pltpu.VMEM((4, 8, 128), F32),
            pltpu.VMEM((2, 64, 128), F32),
            dma((6,)),
            dma,
            dma((4 if n_dev == 64 else 2,)),
            dma,
            dma,
            dma,
            dma,
            dma((3,)),
            dma((3,)),
        ],
        compiler_params=pltpu.CompilerParams(
            collective_id=0, has_side_effects=True, vmem_limit_bytes=48 * 1024 * 1024
        ),
    )(*[pltpu.with_memory_space_constraint(v, pltpu.HBM) for v in (coord, *flat)])
    out, cost = pl.pallas_call(
        finish_kernel,
        grid=(ELEM // 128,),
        out_shape=(
            jax.ShapeDtypeStruct((ELEM, NODES), F32),
            jax.ShapeDtypeStruct((1, 1), F32),
        ),
        in_specs=[
            pl.BlockSpec((NODES, 128), lambda i: (0, i)),
            pl.BlockSpec((1, 128), lambda i: (0, 0)),
        ],
        out_specs=(
            pl.BlockSpec((128, NODES), lambda i: (i, 0)),
            pl.BlockSpec(memory_space=pltpu.SMEM),
        ),
        compiler_params=pltpu.CompilerParams(vmem_limit_bytes=16 * 1024 * 1024),
    )(mid, cost_row)
    return out.reshape(4, 8, 8, NODES), cost.reshape(())


def solution(mesh):
    n_grp, n_dev = mesh.shape["grp"], mesh.shape["dev"]
    rows = P(("grp", "dev"))

    def step(obs_coord, obs_resid, obs_weight, obs_dest, obs_send_slot, obs_elem, obs_slot):
        del obs_slot
        return on_device(
            obs_coord, obs_resid, obs_weight, obs_dest, obs_send_slot, obs_elem, n_grp, n_dev
        )

    return jax.shard_map(
        step,
        mesh=mesh,
        in_specs=(P(None, ("grp", "dev")), rows, rows, rows, rows, rows, rows),
        out_specs=(P("grp", "dev", None, None), P()),
        check_vma=False,
    )
```

```python
import functools
import math

import jax
import jax.numpy as jnp
from jax import lax
from jax.experimental import pallas as pl
from jax.experimental.pallas import tpu as pltpu
from jax.sharding import PartitionSpec as P

CAP = 128
ELEM = 256
NODES = 512
COPLANE = 16
PEERS = 64
NODE_POINTS = [-math.cos(math.pi * k / 7) for k in range(8)]
NODE_SCALE = [
    1.0 / math.prod(NODE_POINTS[a] - NODE_POINTS[m] for m in range(8) if m != a)
    for a in range(8)
]
NT = (((1,), (1,)), ((), ()))
F32, BF16, I32 = jnp.float32, jnp.bfloat16, jnp.int32
EDGE = (0, 7)
OUTER = [(a, b) for a in range(8) for b in range(8) if a in EDGE or b in EDGE]
INNER = [(a, b) for a in range(8) for b in range(8) if not (a in EDGE or b in EDGE)]
OUTER.sort(key=lambda ab: (EDGE.index(ab[0]) if ab[0] in EDGE else 2, ab))
GROUPS = OUTER + INNER
PLACE = {ab: 8 * i for i, ab in enumerate(GROUPS)}
SPLIT = 8 * len(OUTER)


def peer_order(n_dev):
    def hops(offset):
        y, z = offset // COPLANE, (offset % COPLANE) // 2
        return min(y, max(n_dev // COPLANE, 1) - y) + min(z, COPLANE // 2 - z)

    return [0] + sorted(range(1, n_dev), key=lambda o: (hops(o), o))


def bounds_of(n_dev):
    return [0, 16, 32, 48, 56, 64] if n_dev == 64 else [0, 2, 4]


def lanes_of(shape):
    return lax.broadcasted_iota(I32, shape, len(shape) - 1)


def rows_of(shape):
    return lax.broadcasted_iota(I32, shape, len(shape) - 2)


def high_of(value):
    return value.astype(BF16).astype(F32)


def one_hot(ids, count):
    shape = (count, ids.shape[1])
    ids = jnp.broadcast_to(ids, (16, ids.shape[1])).astype(BF16)
    ids = jnp.concatenate([ids] * (count // 16), axis=0)
    row = rows_of(shape).astype(F32).astype(BF16)
    return jnp.where(row == ids, jnp.ones(shape, BF16), jnp.zeros(shape, BF16))


def basis(t):
    shape = (8, t.shape[1])
    t = jnp.broadcast_to(t, shape)
    row = rows_of(shape)
    out = None
    for m in range(8):
        factor = jnp.where(row == m, F32(NODE_SCALE[m]), t - F32(NODE_POINTS[m]))
        out = factor if out is None else out * factor
    return out


def move(x, k):
    return pltpu.roll(x, k % x.shape[1], 1)


def exchange_kernel(
    n_grp, n_dev, coord, resid, weight, dest, slot, elem, mid, cost,
    coord_v, resid_v, weight_v, dest_v, slot_v, elem_v,
    lhs, pick, send, recv, acc, outer, xo, xi, oh,
    c1s, c1r, c2s, c2r, halo_g, halo_d, halo_c, dsend,
    in_sem, send_sem, recv_sem, c1_ssem, c1_rsem, c2_ssem, c2_rsem, h_ssem, h_rsem,
):
    g, d = lax.axis_index("grp"), lax.axis_index("dev")
    co = min(COPLANE, n_dev)
    planes = n_dev // co
    order = peer_order(n_dev)
    here = lax.rem(d, co)
    block = d - here

    def at(dg, dd):
        return {"grp": lax.rem(g + dg + n_grp, n_grp), "dev": lax.rem(d + dd + n_dev, n_dev)}

    loads = [
        pltpu.make_async_copy(src, dst, in_sem.at[i])
        for i, (src, dst) in enumerate(
            [(dest, dest_v), (slot, slot_v), (elem, elem_v), (coord, coord_v), (resid, resid_v), (weight, weight_v)]
        )
    ]
    for load in loads:
        load.start()

    barrier = pltpu.get_barrier_semaphore()
    corners = [(-1, -1), (-1, 1), (1, -1), (1, 1)]
    peers = [(k, p * co) for k in range(1, n_grp) for p in range(planes)]
    peers += corners
    peers += [(0, o) for o in order[1:]]
    for dg, dd in reversed(peers):
        pl.semaphore_signal(barrier, inc=1, device_id=at(dg, dd))
    for load in loads:
        load.wait()

    for j in range(resid_v.shape[0] // 2):
        def pair(ref):
            return jnp.concatenate([ref[2 * j : 2 * j + 1, :], ref[2 * j + 1 : 2 * j + 2, :]], axis=1)

        cols = slice(256 * j, 256 * j + 256)
        to = pair(dest_v)
        upper = to >> 5
        mask = one_hot((to - 32 * upper).astype(F32), 32)
        pick[:, cols] = one_hot((upper * CAP + pair(slot_v)).astype(F32), 256)
        parts = []
        for value in [coord_v[c : c + 1, cols] for c in range(3)] + [pair(weight_v) * pair(resid_v)]:
            high = high_of(value)
            parts += [high, value - high]
        parts.append(pair(elem_v).astype(F32))
        for i, part in enumerate(parts):
            wide = jnp.broadcast_to(part, (16, 256)).astype(BF16)
            lhs[32 * i : 32 * i + 32, cols] = mask * jnp.concatenate([wide, wide], axis=0)
    packed = lax.dot_general(lhs[...], pick[...], NT, preferred_element_type=F32)
    part = [packed[32 * k : 32 * k + 32] for k in range(9)]
    values = [part[2 * c] + part[2 * c + 1] for c in range(4)] + [part[8]]
    for c, value in enumerate(values):
        send[0:32, c, :] = value[:, :CAP]
        send[32:64, c, :] = value[:, CAP:]
    r = resid_v[...]
    c1s[...] = jnp.sum(weight_v[...] * r * r, axis=0, keepdims=True)

    recv[0] = send[d]
    c1r[here] = c1s[...]

    pl.semaphore_wait(barrier, len(peers))

    bounds = bounds_of(n_dev)
    chunks = list(zip(bounds[:-1], bounds[1:]))
    chunk_of = [i for i, (first, last) in enumerate(chunks) for _ in range(first, last)]

    def message(k):
        to = lax.rem(d + order[k], n_dev)
        return pltpu.make_async_remote_copy(
            src_ref=send.at[to],
            dst_ref=recv.at[k],
            send_sem=send_sem,
            recv_sem=recv_sem.at[chunk_of[k]],
            device_id={"grp": g, "dev": to},
        )

    def await_bytes(ref, sem):
        pltpu.make_async_copy(ref, ref, sem).wait()

    for k in range(1, n_dev):
        message(k).start()

    def partial_one(k):
        return pltpu.make_async_remote_copy(
            src_ref=c1s, dst_ref=c1r.at[here], send_sem=c1_ssem, recv_sem=c1_rsem,
            device_id={"grp": g, "dev": block + lax.rem(here + k, co)},
        )

    for k in range(1, co):
        partial_one(k).start()

    mine = g * planes + block // co
    rest = [(k, p) for k in range(n_grp) for p in range(planes) if k or p]
    twos = [
        pltpu.make_async_remote_copy(
            src_ref=c2s, dst_ref=c2r.at[mine], send_sem=c2_ssem, recv_sem=c2_rsem,
            device_id=at(k, p * co),
        )
        for k, p in rest
    ]

    def build(i, p):
        first, second = recv[2 * p], recv[2 * p + 1]

        def row(c):
            return jnp.concatenate([first[c : c + 1], second[c : c + 1]], axis=1)

        begin = 256 * p - CAP * chunks[i][0]
        cols = slice(begin, begin + 256)
        fa = basis(row(0)) * row(3)
        fb = basis(row(1))
        fc = basis(row(2))
        bc = [fb[b : b + 1] * fc for b in range(8)]
        for k in range(0, 64, 2):
            full = jnp.concatenate([fa[a : a + 1] * bc[b] for a, b in GROUPS[k : k + 2]], axis=0)
            high = full.astype(BF16)
            low = (full - high.astype(F32)).astype(BF16)
            ref, row_of, count = (xo[i], 8 * k, SPLIT) if 8 * k < SPLIT else (xi[i], 8 * k - SPLIT, NODES - SPLIT)
            ref[row_of : row_of + 16, cols] = high
            ref[count + row_of : count + row_of + 16, cols] = low
        oh[i][:, cols] = one_hot(row(4), ELEM)

    def product(ref, i):
        return lax.dot_general(ref[i][...], oh[i][...], NT, preferred_element_type=F32)

    def arrived(i):
        first, last = max(chunks[i][0], 1), chunks[i][1]
        await_bytes(recv.at[first:last], recv_sem.at[i])

    def block_of(body):
        pl.when(d >= 0)(body)

    for i in range(len(chunks)):
        arrived(i)

        @block_of
        def _():
            for p in range(chunks[i][0] // 2, chunks[i][1] // 2):
                build(i, p)
            now = product(xo, i)
            if i > 0:
                now = acc[...] + now
            if i + 1 < len(chunks):
                acc[...] = now
            else:
                outer[...] = now[:SPLIT] + now[SPLIT:]

        if i == 1:
            await_bytes(c1r.at[1:co], c1_rsem)
            total = c1r[0]
            for k in range(1, co):
                total += c1r[k]
            c2s[...] = total
            c2r[mine] = total
            for m in twos:
                m.start()

    lane = lanes_of((8, ELEM))

    def rg(ref, a, b):
        return ref[PLACE[a, b] : PLACE[a, b] + 8, :]

    def put(ref, a, b, value):
        ref[PLACE[a, b] : PLACE[a, b] + 8, :] = value

    for b in range(8):
        low, high = rg(outer, 0, b), rg(outer, 7, b)
        put(outer, 0, b, low + jnp.where(lane >= 64, move(high, 64), 0.0))
        put(outer, 7, b, high + jnp.where(lane < 192, move(low, -64), 0.0))
    half = lanes_of((8, 128))
    for a in range(8):
        for side, b in ((0, 0), (1, 7)):
            plane = rg(outer, a, b)
            near = ((half >> 3) & 7) == b
            left = jnp.where(near, plane[:, :128], 0.0)
            right = jnp.where(near, plane[:, 128:], 0.0)
            dsend[side, 8 * a : 8 * a + 8, :] = left + move(right, 8 if b == 0 else -8)

    def halo(kind, src, dst, dg, dd):
        return pltpu.make_async_remote_copy(
            src_ref=src, dst_ref=dst, send_sem=h_ssem.at[kind], recv_sem=h_rsem.at[kind],
            device_id=at(dg, dd),
        )

    def tile(a, b, count, right):
        first = PLACE[a, b]
        return outer.at[first : first + 8 * count, (128 if right else 0) : (256 if right else 128)]

    halos = [
        halo(0, tile(0, 0, 8, False), halo_g.at[0], -1, 0),
        halo(0, tile(7, 0, 8, True), halo_g.at[1], 1, 0),
        halo(1, dsend.at[0], halo_d.at[0], 0, -1),
        halo(1, dsend.at[1], halo_d.at[1], 0, 1),
        halo(2, tile(0, 0, 1, False), halo_c.at[0], -1, -1),
        halo(2, tile(0, 7, 1, False), halo_c.at[1], -1, 1),
        halo(2, tile(7, 0, 1, True), halo_c.at[2], 1, -1),
        halo(2, tile(7, 7, 1, True), halo_c.at[3], 1, 1),
    ]
    for m in halos:
        m.start()
    @block_of
    def _():
        left = sum(product(xi, i) for i in range(len(chunks)))
        mid[SPLIT:, :] = left[: NODES - SPLIT] + left[NODES - SPLIT :]


    for kind, ref in enumerate((halo_g, halo_d, halo_c)):
        await_bytes(ref, h_rsem.at[kind])

    up_g, down_g = g > 0, g < n_grp - 1
    up_d, down_d = d > 0, d < n_dev - 1
    ey = (lane >> 3) & 7

    def wide(value):
        return jnp.concatenate([value, value], axis=1)

    planes_now = {ab: rg(outer, *ab) for ab in OUTER}
    for b in range(8):
        from_low = move(halo_g[1, 8 * b : 8 * b + 8, :], 64)
        from_high = move(halo_g[0, 8 * b : 8 * b + 8, :], 64)
        planes_now[0, b] += jnp.where((lane < 64) & up_g, wide(from_low), 0.0)
        planes_now[7, b] += jnp.where((lane >= 192) & down_g, wide(from_high), 0.0)
    for a in range(8):
        low, high = planes_now[a, 0], planes_now[a, 7]
        theirs = halo_d[1, 8 * a : 8 * a + 8, :]
        to_low = jnp.concatenate([move(theirs, -56), move(theirs, -48)], axis=1)
        theirs = halo_d[0, 8 * a : 8 * a + 8, :]
        to_high = jnp.concatenate([move(theirs, 56), move(theirs, 48)], axis=1)
        if a == 0:
            to_low += jnp.where((lane < 8) & up_g, wide(move(halo_c[3], -120)), 0.0)
            to_high += jnp.where((lane >= 56) & (lane < 64) & up_g, wide(move(halo_c[2], -8)), 0.0)
        if a == 7:
            to_low += jnp.where((lane >= 192) & (lane < 200) & down_g, wide(move(halo_c[1], 8)), 0.0)
            to_high += jnp.where((lane >= 248) & down_g, wide(move(halo_c[0], 120)), 0.0)
        new_low = jnp.where(ey > 0, move(high, 8), jnp.where(up_d, to_low, 0.0))
        new_high = jnp.where(ey < 7, move(low, -8), jnp.where(down_d, to_high, 0.0))
        planes_now[a, 0] = low + new_low
        planes_now[a, 7] = high + new_high
    for ab in OUTER:
        put(mid, *ab, planes_now[ab])

    await_bytes(c2r.at[1:], c2_rsem)
    total = c2r[0]
    for k in range(1, n_grp * planes):
        total += c2r[k]
    cost[...] = total
    await_bytes(recv.at[1:], send_sem)
    await_bytes(c1r.at[1:], c1_ssem)
    await_bytes(c2r.at[1:], c2_ssem)
    for kind, ref in enumerate((halo_g, halo_d, halo_c)):
        await_bytes(ref, h_ssem.at[kind])


def finish_kernel(mid, cost_row, out, cost):
    shape = (8, 128)
    ez = lanes_of(shape) & 7
    row = rows_of(shape)
    done = {}
    for ab in GROUPS:
        now = mid[PLACE[ab] : PLACE[ab] + 8, :]
        z = jnp.where(row == 7, move(now, 1), move(now, -1))
        to_low = jnp.where((row == 0) & (ez > 0), pltpu.roll(z, 1, 0), 0.0)
        to_high = jnp.where((row == 7) & (ez < 7), pltpu.roll(z, 7, 0), 0.0)
        done[ab] = now + to_low + to_high
    for a in range(0, 8, 2):
        both = jnp.concatenate([done[k, b] for k in (a, a + 1) for b in range(8)], axis=0)
        out[:, 64 * a : 64 * a + 128] = both.T
    cost[0, 0] = 0.5 * jnp.sum(cost_row[...])


def on_device(coord, resid, weight, dest, slot, elem, n_grp, n_dev):
    rows = resid.shape[0] // 128
    flat = [v.reshape(rows, 128) for v in (resid, weight, dest, slot, elem)]
    co = min(COPLANE, n_dev)
    blocks = n_grp * (n_dev // co)
    dma = pltpu.SemaphoreType.DMA
    bounds = bounds_of(n_dev)
    widths = [CAP * (last - first) for first, last in zip(bounds[:-1], bounds[1:])]
    vmem = pl.BlockSpec(memory_space=pltpu.VMEM)
    mid, cost_row = pl.pallas_call(
        functools.partial(exchange_kernel, n_grp, n_dev),
        out_shape=(
            jax.ShapeDtypeStruct((NODES, ELEM), F32),
            jax.ShapeDtypeStruct((1, 128), F32),
        ),
        in_specs=[pl.BlockSpec(memory_space=pltpu.HBM)] * 6,
        out_specs=(vmem, vmem),
        scratch_shapes=[
            pltpu.VMEM(coord.shape, F32),
            pltpu.VMEM((rows, 128), F32),
            pltpu.VMEM((rows, 128), F32),
            pltpu.VMEM((rows, 128), I32),
            pltpu.VMEM((rows, 128), I32),
            pltpu.VMEM((rows, 128), I32),
            pltpu.VMEM((9 * 32, rows * 128), BF16),
            pltpu.VMEM((256, rows * 128), BF16),
            pltpu.VMEM((PEERS, 5, CAP), F32),
            pltpu.VMEM((n_dev, 5, CAP), F32),
            pltpu.VMEM((2 * SPLIT, ELEM), F32),
            pltpu.VMEM((SPLIT, ELEM), F32),
            [pltpu.VMEM((2 * SPLIT, n), BF16) for n in widths],
            [pltpu.VMEM((2 * (NODES - SPLIT), n), BF16) for n in widths],
            [pltpu.VMEM((ELEM, n), BF16) for n in widths],
            pltpu.VMEM((1, 128), F32),
            pltpu.VMEM((co, 1, 128), F32),
            pltpu.VMEM((1, 128), F32),
            pltpu.VMEM((blocks, 1, 128), F32),
            pltpu.VMEM((2, 64, 128), F32),
            pltpu.VMEM((2, 64, 128), F32),
            pltpu.VMEM((4, 8, 128), F32),
            pltpu.VMEM((2, 64, 128), F32),
            dma((6,)),
            dma,
            dma((len(widths),)),
            dma,
            dma,
            dma,
            dma,
            dma((3,)),
            dma((3,)),
        ],
        compiler_params=pltpu.CompilerParams(
            collective_id=0, has_side_effects=True, vmem_limit_bytes=48 * 1024 * 1024
        ),
    )(*[pltpu.with_memory_space_constraint(v, pltpu.HBM) for v in (coord, *flat)])
    out, cost = pl.pallas_call(
        finish_kernel,
        grid=(ELEM // 128,),
        out_shape=(
            jax.ShapeDtypeStruct((ELEM, NODES), F32),
            jax.ShapeDtypeStruct((1, 1), F32),
        ),
        in_specs=[
            pl.BlockSpec((NODES, 128), lambda i: (0, i)),
            pl.BlockSpec((1, 128), lambda i: (0, 0)),
        ],
        out_specs=(
            pl.BlockSpec((128, NODES), lambda i: (i, 0)),
            pl.BlockSpec(memory_space=pltpu.SMEM),
        ),
        compiler_params=pltpu.CompilerParams(vmem_limit_bytes=16 * 1024 * 1024),
    )(mid, cost_row)
    return out.reshape(4, 8, 8, NODES), cost.reshape(())


def solution(mesh):
    n_grp, n_dev = mesh.shape["grp"], mesh.shape["dev"]
    rows = P(("grp", "dev"))

    def step(obs_coord, obs_resid, obs_weight, obs_dest, obs_send_slot, obs_elem, obs_slot):
        del obs_slot
        return on_device(
            obs_coord, obs_resid, obs_weight, obs_dest, obs_send_slot, obs_elem, n_grp, n_dev
        )

    return jax.shard_map(
        step,
        mesh=mesh,
        in_specs=(P(None, ("grp", "dev")), rows, rows, rows, rows, rows, rows),
        out_specs=(P("grp", "dev", None, None), P()),
        check_vma=False,
    )
```

```python
import functools
import math

import jax
import jax.numpy as jnp
from jax import lax
from jax.experimental import pallas as pl
from jax.experimental.pallas import tpu as pltpu
from jax.sharding import PartitionSpec as P

CAP = 128
ELEM = 256
NODES = 512
COPLANE = 16
PEERS = 64
NODE_POINTS = [-math.cos(math.pi * k / 7) for k in range(8)]
NODE_SCALE = [
    1.0 / math.prod(NODE_POINTS[a] - NODE_POINTS[m] for m in range(8) if m != a)
    for a in range(8)
]
NT = (((1,), (1,)), ((), ()))
F32, BF16, I32 = jnp.float32, jnp.bfloat16, jnp.int32
EDGE = (0, 7)
OUTER = [(a, b) for a in range(8) for b in range(8) if a in EDGE or b in EDGE]
INNER = [(a, b) for a in range(8) for b in range(8) if not (a in EDGE or b in EDGE)]
OUTER.sort(key=lambda ab: (EDGE.index(ab[0]) if ab[0] in EDGE else 2, ab))
GROUPS = OUTER + INNER
PLACE = {ab: 8 * i for i, ab in enumerate(GROUPS)}
SPLIT = 8 * len(OUTER)


def peer_order(n_dev):
    def hops(offset):
        y, z = offset // COPLANE, (offset % COPLANE) // 2
        return min(y, max(n_dev // COPLANE, 1) - y) + min(z, COPLANE // 2 - z)

    return [0] + sorted(range(1, n_dev), key=lambda o: (hops(o), o))


def bounds_of(n_dev):
    return [0, 16, 32, 48, 60, 64] if n_dev == 64 else [0, 2, 4]


def lanes_of(shape):
    return lax.broadcasted_iota(I32, shape, len(shape) - 1)


def rows_of(shape):
    return lax.broadcasted_iota(I32, shape, len(shape) - 2)


def high_of(value):
    return value.astype(BF16).astype(F32)


def one_hot(ids, count):
    shape = (count, ids.shape[1])
    ids = jnp.broadcast_to(ids, (16, ids.shape[1])).astype(BF16)
    ids = jnp.concatenate([ids] * (count // 16), axis=0)
    row = rows_of(shape).astype(F32).astype(BF16)
    return jnp.where(row == ids, jnp.ones(shape, BF16), jnp.zeros(shape, BF16))


def basis(t):
    shape = (8, t.shape[1])
    t = jnp.broadcast_to(t, shape)
    row = rows_of(shape)
    out = None
    for m in range(8):
        factor = jnp.where(row == m, F32(NODE_SCALE[m]), t - F32(NODE_POINTS[m]))
        out = factor if out is None else out * factor
    return out


def move(x, k):
    return pltpu.roll(x, k % x.shape[1], 1)


def exchange_kernel(
    n_grp, n_dev, coord, resid, weight, dest, slot, elem, mid, cost,
    coord_v, resid_v, weight_v, dest_v, slot_v, elem_v,
    lhs, pick, send, recv, acc, outer, summed, bases, xo, xi, oh,
    c1s, c1r, c2s, c2r, halo_g, halo_d, halo_c, gsend, dsend,
    in_sem, send_sem, recv_sem, c1_ssem, c1_rsem, c2_ssem, c2_rsem, h_ssem, h_rsem,
):
    g, d = lax.axis_index("grp"), lax.axis_index("dev")
    co = min(COPLANE, n_dev)
    planes = n_dev // co
    order = peer_order(n_dev)
    here = lax.rem(d, co)
    block = d - here

    def at(dg, dd):
        return {"grp": lax.rem(g + dg + n_grp, n_grp), "dev": lax.rem(d + dd + n_dev, n_dev)}

    loads = [
        pltpu.make_async_copy(src, dst, in_sem.at[i])
        for i, (src, dst) in enumerate(
            [(dest, dest_v), (slot, slot_v), (elem, elem_v), (coord, coord_v), (resid, resid_v), (weight, weight_v)]
        )
    ]
    barrier = pltpu.get_barrier_semaphore()
    corners = [(-1, -1), (-1, 1), (1, -1), (1, 1)]
    peers = [(k, p * co) for k in range(1, n_grp) for p in range(planes)]
    peers += corners
    peers += [(0, o) for o in order[1:]]
    for i, (dg, dd) in enumerate(reversed(peers)):
        if i == len(peers) // 2:
            for load in loads:
                load.start()
        pl.semaphore_signal(barrier, inc=1, device_id=at(dg, dd))
    for load in loads:
        load.wait()

    for j in range(resid_v.shape[0] // 2):
        def pair(ref):
            return jnp.concatenate([ref[2 * j : 2 * j + 1, :], ref[2 * j + 1 : 2 * j + 2, :]], axis=1)

        cols = slice(256 * j, 256 * j + 256)
        to = pair(dest_v)
        upper = to >> 5
        mask = one_hot((to - 32 * upper).astype(F32), 32)
        pick[:, cols] = one_hot((upper * CAP + pair(slot_v)).astype(F32), 256)
        parts = []
        for value in [coord_v[c : c + 1, cols] for c in range(3)] + [pair(weight_v) * pair(resid_v)]:
            high = high_of(value)
            parts += [high, value - high]
        parts.append(pair(elem_v).astype(F32))
        for i, part in enumerate(parts):
            wide = jnp.broadcast_to(part, (16, 256)).astype(BF16)
            lhs[32 * i : 32 * i + 32, cols] = mask * jnp.concatenate([wide, wide], axis=0)
    packed = lax.dot_general(lhs[...], pick[...], NT, preferred_element_type=F32)
    part = [packed[32 * k : 32 * k + 32] for k in range(9)]
    values = [part[2 * c] + part[2 * c + 1] for c in range(4)] + [part[8]]
    for c, value in enumerate(values):
        send[0:32, c, :] = value[:, :CAP]
        send[32:64, c, :] = value[:, CAP:]
    r = resid_v[...]
    c1s[...] = jnp.sum(weight_v[...] * r * r, axis=0, keepdims=True)

    recv[0] = send[d]
    c1r[here] = c1s[...]

    pl.semaphore_wait(barrier, len(peers))

    bounds = bounds_of(n_dev)
    chunks = list(zip(bounds[:-1], bounds[1:]))
    chunk_of = [i for i, (first, last) in enumerate(chunks) for _ in range(first, last)]

    def message(k):
        to = lax.rem(d + order[k], n_dev)
        return pltpu.make_async_remote_copy(
            src_ref=send.at[to],
            dst_ref=recv.at[k],
            send_sem=send_sem,
            recv_sem=recv_sem.at[chunk_of[k]],
            device_id={"grp": g, "dev": to},
        )

    def await_bytes(ref, sem):
        pltpu.make_async_copy(ref, ref, sem).wait()

    def partial_one(k):
        return pltpu.make_async_remote_copy(
            src_ref=c1s, dst_ref=c1r.at[here], send_sem=c1_ssem, recv_sem=c1_rsem,
            device_id={"grp": g, "dev": block + lax.rem(here + k, co)},
        )

    for k in range(1, co):
        partial_one(k).start()
    for k in range(1, n_dev):
        message(k).start()

    mine = g * planes + block // co
    rest = [(k, p) for k in range(n_grp) for p in range(planes) if k or p]
    twos = [
        pltpu.make_async_remote_copy(
            src_ref=c2s, dst_ref=c2r.at[mine], send_sem=c2_ssem, recv_sem=c2_rsem,
            device_id=at(k, p * co),
        )
        for k, p in rest
    ]

    def rows_built(ref, cols, groups, fa, fb, fc):
        bc = [fb[b : b + 1] * fc for b in range(8)]
        count = 8 * len(groups)
        for k in range(0, len(groups), 2):
            full = jnp.concatenate([fa[a : a + 1] * bc[b] for a, b in groups[k : k + 2]], axis=0)
            high = full.astype(BF16)
            low = (full - high.astype(F32)).astype(BF16)
            ref[8 * k : 8 * k + 16, cols] = high
            ref[count + 8 * k : count + 8 * k + 16, cols] = low

    def cols_of(i, p):
        begin = 256 * p - CAP * chunks[i][0]
        return slice(begin, begin + 256)

    def build(i, p):
        first, second = recv[2 * p], recv[2 * p + 1]

        def row(c):
            return jnp.concatenate([first[c : c + 1], second[c : c + 1]], axis=1)

        cols = cols_of(i, p)
        fa = basis(row(0)) * row(3)
        fb = basis(row(1))
        fc = basis(row(2))
        for c, value in enumerate((fa, fb, fc)):
            bases[c, p] = value
        rows_built(xo[i], cols, OUTER, fa, fb, fc)
        oh[i][:, cols] = one_hot(row(4), ELEM)

    def product(ref, i):
        return lax.dot_general(ref[i][...], oh[i][...], NT, preferred_element_type=F32)

    def arrived(i):
        first, last = max(chunks[i][0], 1), chunks[i][1]
        await_bytes(recv.at[first:last], recv_sem.at[i])

    def block_of(body):
        pl.when(d >= 0)(body)

    for i in range(len(chunks)):
        arrived(i)

        @block_of
        def _():
            for p in range(chunks[i][0] // 2, chunks[i][1] // 2):
                build(i, p)
            now = product(xo, i)
            if i > 0:
                now = acc[...] + now
            if i + 1 < len(chunks):
                acc[...] = now
            else:
                outer[...] = now[:SPLIT] + now[SPLIT:]

        if i == 1:
            await_bytes(c1r.at[1:co], c1_rsem)
            total = c1r[0]
            for k in range(1, co):
                total += c1r[k]
            c2s[...] = total
            c2r[mine] = total
            for m in twos:
                m.start()

    def halo(kind, src, dst, dg, dd):
        return pltpu.make_async_remote_copy(
            src_ref=src, dst_ref=dst, send_sem=h_ssem.at[kind], recv_sem=h_rsem.at[kind],
            device_id=at(dg, dd),
        )

    def line(a, b):
        first, half = PLACE[a, b], 128 if a else 0
        return outer.at[first : first + 8, half : half + 128]

    for i, (dg, dd) in enumerate(corners):
        halo(2, line(0 if dg < 0 else 7, 0 if dd < 0 else 7), halo_c.at[i], dg, dd).start()

    lane = lanes_of((8, ELEM))
    half = lanes_of((8, 128))

    def rg(ref, a, b):
        return ref[PLACE[a, b] : PLACE[a, b] + 8, :]

    def put(ref, a, b, value):
        ref[PLACE[a, b] : PLACE[a, b] + 8, :] = value

    now = {ab: rg(outer, *ab) for ab in OUTER}
    for b in (0, 7, 1, 2, 3, 4, 5, 6):
        low, high = now[0, b], now[7, b]
        now[0, b] = low + jnp.where(lane >= 64, move(high, 64), 0.0)
        now[7, b] = high + jnp.where(lane < 192, move(low, -64), 0.0)
        put(summed, 0, b, now[0, b])
        put(summed, 7, b, now[7, b])
    for side, b, step in ((0, 0, 8), (1, 7, -8)):
        near = ((half >> 3) & 7) == b
        for first in (0, 4):
            packed_planes = None
            for j in range(4):
                plane = now[first + j, b]
                left = jnp.where(near, plane[:, :128], 0.0)
                right = jnp.where(near, plane[:, 128:], 0.0)
                piece = move(left + move(right, step), 2 * step * j)
                packed_planes = piece if j == 0 else packed_planes + piece
            dsend[side, 2 * first : 2 * first + 8, :] = packed_planes
    for side, dd in enumerate((-1, 1)):
        halo(1, dsend.at[side], halo_d.at[side], 0, dd).start()
    for b in range(4):
        gsend[0, 8 * b : 8 * b + 8, :] = jnp.where(
            half < 64, rg(outer, 0, b)[:, :128], move(rg(outer, 0, b + 4)[:, :128], 64)
        )
        gsend[1, 8 * b : 8 * b + 8, :] = jnp.where(
            half < 64, move(rg(outer, 7, b)[:, 128:], 64), rg(outer, 7, b + 4)[:, 128:]
        )
    for side, dg in enumerate((-1, 1)):
        halo(0, gsend.at[side], halo_g.at[side], dg, 0).start()

    @block_of
    def _():
        left = None
        for i, (first, last) in enumerate(chunks):
            for p in range(first // 2, last // 2):
                rows_built(xi[i], cols_of(i, p), INNER, *[bases[c, p] for c in range(3)])
            now = product(xi, i)
            left = now if left is None else left + now
        mid[SPLIT:, :] = left[: NODES - SPLIT] + left[NODES - SPLIT :]


    for kind, ref in enumerate((halo_g, halo_d, halo_c)):
        await_bytes(ref, h_rsem.at[kind])

    up_g, down_g = g > 0, g < n_grp - 1
    up_d, down_d = d > 0, d < n_dev - 1
    ey = (lane >> 3) & 7

    def wide(value):
        return jnp.concatenate([value, value], axis=1)

    planes_now = {(a, b): rg(summed if a in EDGE else outer, a, b) for a, b in OUTER}
    for b in range(8):
        part = slice(8 * (b % 4), 8 * (b % 4) + 8)
        from_low, from_high = halo_g[1, part, :], halo_g[0, part, :]
        if b < 4:
            from_high = move(from_high, 64)
        else:
            from_low = move(from_low, 64)
        planes_now[0, b] += jnp.where((lane < 64) & up_g, wide(from_low), 0.0)
        planes_now[7, b] += jnp.where((lane >= 192) & down_g, wide(from_high), 0.0)
    for a in range(8):
        low, high = planes_now[a, 0], planes_now[a, 7]
        part, shift = slice(8 * (a // 4), 8 * (a // 4) + 8), 16 * (a % 4)
        theirs = halo_d[1, part, :]
        to_low = jnp.concatenate([move(theirs, shift - 56), move(theirs, shift - 48)], axis=1)
        theirs = halo_d[0, part, :]
        to_high = jnp.concatenate([move(theirs, 56 - shift), move(theirs, 48 - shift)], axis=1)
        if a == 0:
            to_low += jnp.where((lane < 8) & up_g, wide(move(halo_c[3], -120)), 0.0)
            to_high += jnp.where((lane >= 56) & (lane < 64) & up_g, wide(move(halo_c[2], -8)), 0.0)
        if a == 7:
            to_low += jnp.where((lane >= 192) & (lane < 200) & down_g, wide(move(halo_c[1], 8)), 0.0)
            to_high += jnp.where((lane >= 248) & down_g, wide(move(halo_c[0], 120)), 0.0)
        new_low = jnp.where(ey > 0, move(high, 8), jnp.where(up_d, to_low, 0.0))
        new_high = jnp.where(ey < 7, move(low, -8), jnp.where(down_d, to_high, 0.0))
        planes_now[a, 0] = low + new_low
        planes_now[a, 7] = high + new_high
    for ab in OUTER:
        put(mid, *ab, planes_now[ab])

    await_bytes(c2r.at[1:], c2_rsem)
    total = c2r[0]
    for k in range(1, n_grp * planes):
        total += c2r[k]
    cost[...] = total
    await_bytes(recv.at[1:], send_sem)
    await_bytes(c1r.at[1:], c1_ssem)
    await_bytes(c2r.at[1:], c2_ssem)
    for kind, ref in enumerate((halo_g, halo_d, halo_c)):
        await_bytes(ref, h_ssem.at[kind])


def finish_kernel(mid, cost_row, out, cost):
    shape = (8, 128)
    ez = lanes_of(shape) & 7
    row = rows_of(shape)
    done = {}
    for ab in GROUPS:
        now = mid[PLACE[ab] : PLACE[ab] + 8, :]
        z = jnp.where(row == 7, move(now, 1), move(now, -1))
        to_low = jnp.where((row == 0) & (ez > 0), pltpu.roll(z, 1, 0), 0.0)
        to_high = jnp.where((row == 7) & (ez < 7), pltpu.roll(z, 7, 0), 0.0)
        done[ab] = now + to_low + to_high
    for a in range(0, 8, 2):
        both = jnp.concatenate([done[k, b] for k in (a, a + 1) for b in range(8)], axis=0)
        out[:, 64 * a : 64 * a + 128] = both.T
    cost[0, 0] = 0.5 * jnp.sum(cost_row[...])


def on_device(coord, resid, weight, dest, slot, elem, n_grp, n_dev):
    rows = resid.shape[0] // 128
    flat = [v.reshape(rows, 128) for v in (resid, weight, dest, slot, elem)]
    co = min(COPLANE, n_dev)
    blocks = n_grp * (n_dev // co)
    dma = pltpu.SemaphoreType.DMA
    bounds = bounds_of(n_dev)
    widths = [CAP * (last - first) for first, last in zip(bounds[:-1], bounds[1:])]
    vmem = pl.BlockSpec(memory_space=pltpu.VMEM)
    mid, cost_row = pl.pallas_call(
        functools.partial(exchange_kernel, n_grp, n_dev),
        out_shape=(
            jax.ShapeDtypeStruct((NODES, ELEM), F32),
            jax.ShapeDtypeStruct((1, 128), F32),
        ),
        in_specs=[pl.BlockSpec(memory_space=pltpu.HBM)] * 6,
        out_specs=(vmem, vmem),
        scratch_shapes=[
            pltpu.VMEM(coord.shape, F32),
            pltpu.VMEM((rows, 128), F32),
            pltpu.VMEM((rows, 128), F32),
            pltpu.VMEM((rows, 128), I32),
            pltpu.VMEM((rows, 128), I32),
            pltpu.VMEM((rows, 128), I32),
            pltpu.VMEM((9 * 32, rows * 128), BF16),
            pltpu.VMEM((256, rows * 128), BF16),
            pltpu.VMEM((PEERS, 5, CAP), F32),
            pltpu.VMEM((n_dev, 5, CAP), F32),
            pltpu.VMEM((2 * SPLIT, ELEM), F32),
            pltpu.VMEM((SPLIT, ELEM), F32),
            pltpu.VMEM((128, ELEM), F32),
            pltpu.VMEM((3, n_dev // 2, 8, 256), F32),
            [pltpu.VMEM((2 * SPLIT, n), BF16) for n in widths],
            [pltpu.VMEM((2 * (NODES - SPLIT), n), BF16) for n in widths],
            [pltpu.VMEM((ELEM, n), BF16) for n in widths],
            pltpu.VMEM((1, 128), F32),
            pltpu.VMEM((co, 1, 128), F32),
            pltpu.VMEM((1, 128), F32),
            pltpu.VMEM((blocks, 1, 128), F32),
            pltpu.VMEM((2, 32, 128), F32),
            pltpu.VMEM((2, 16, 128), F32),
            pltpu.VMEM((4, 8, 128), F32),
            pltpu.VMEM((2, 32, 128), F32),
            pltpu.VMEM((2, 16, 128), F32),
            dma((6,)),
            dma,
            dma((len(widths),)),
            dma,
            dma,
            dma,
            dma,
            dma((3,)),
            dma((3,)),
        ],
        compiler_params=pltpu.CompilerParams(
            collective_id=0, has_side_effects=True, vmem_limit_bytes=48 * 1024 * 1024
        ),
    )(*[pltpu.with_memory_space_constraint(v, pltpu.HBM) for v in (coord, *flat)])
    out, cost = pl.pallas_call(
        finish_kernel,
        grid=(ELEM // 128,),
        out_shape=(
            jax.ShapeDtypeStruct((ELEM, NODES), F32),
            jax.ShapeDtypeStruct((1, 1), F32),
        ),
        in_specs=[
            pl.BlockSpec((NODES, 128), lambda i: (0, i)),
            pl.BlockSpec((1, 128), lambda i: (0, 0)),
        ],
        out_specs=(
            pl.BlockSpec((128, NODES), lambda i: (i, 0)),
            pl.BlockSpec(memory_space=pltpu.SMEM),
        ),
        compiler_params=pltpu.CompilerParams(vmem_limit_bytes=16 * 1024 * 1024),
    )(mid, cost_row)
    return out.reshape(4, 8, 8, NODES), cost.reshape(())


def solution(mesh):
    n_grp, n_dev = mesh.shape["grp"], mesh.shape["dev"]
    rows = P(("grp", "dev"))

    def step(obs_coord, obs_resid, obs_weight, obs_dest, obs_send_slot, obs_elem, obs_slot):
        del obs_slot
        return on_device(
            obs_coord, obs_resid, obs_weight, obs_dest, obs_send_slot, obs_elem, n_grp, n_dev
        )

    return jax.shard_map(
        step,
        mesh=mesh,
        in_specs=(P(None, ("grp", "dev")), rows, rows, rows, rows, rows, rows),
        out_specs=(P("grp", "dev", None, None), P()),
        check_vma=False,
    )
```

```python
import functools
import math

import jax
import jax.numpy as jnp
from jax import lax
from jax.experimental import pallas as pl
from jax.experimental.pallas import tpu as pltpu
from jax.sharding import PartitionSpec as P

CAP = 128
ELEM = 256
NODES = 512
COPLANE = 16
PEERS = 64
NODE_POINTS = [-math.cos(math.pi * k / 7) for k in range(8)]
NODE_SCALE = [
    1.0 / math.prod(NODE_POINTS[a] - NODE_POINTS[m] for m in range(8) if m != a)
    for a in range(8)
]
NT = (((1,), (1,)), ((), ()))
F32, BF16, I32 = jnp.float32, jnp.bfloat16, jnp.int32
EDGE = (0, 7)
OUTER = [(a, b) for a in range(8) for b in range(8) if a in EDGE or b in EDGE]
INNER = [(a, b) for a in range(8) for b in range(8) if not (a in EDGE or b in EDGE)]
OUTER.sort(key=lambda ab: (EDGE.index(ab[0]) if ab[0] in EDGE else 2, ab))
GROUPS = OUTER + INNER
PLACE = {ab: 8 * i for i, ab in enumerate(GROUPS)}
SPLIT = 8 * len(OUTER)


def peer_steps(n_dev):
    size_y, size_z = n_dev // min(COPLANE, n_dev), min(COPLANE, n_dev) // 2
    steps = [(y, z, c) for y in range(size_y) for z in range(size_z) for c in range(2)]

    def hops(step):
        y, z, _ = step
        return min(y, size_y - y) + min(z, size_z - z)

    return sorted(steps, key=lambda step: (hops(step), step))


def bounds_of(n_dev):
    return [0, 8, 24, 40, 52, 64] if n_dev == 64 else [0, 2, 4]


def lanes_of(shape):
    return lax.broadcasted_iota(I32, shape, len(shape) - 1)


def rows_of(shape):
    return lax.broadcasted_iota(I32, shape, len(shape) - 2)


def high_of(value):
    return value.astype(BF16).astype(F32)


def one_hot(ids, count):
    shape = (count, ids.shape[1])
    ids = jnp.broadcast_to(ids, (16, ids.shape[1])).astype(BF16)
    ids = jnp.concatenate([ids] * (count // 16), axis=0)
    row = rows_of(shape).astype(F32).astype(BF16)
    return jnp.where(row == ids, jnp.ones(shape, BF16), jnp.zeros(shape, BF16))


def basis(t):
    shape = (8, t.shape[1])
    t = jnp.broadcast_to(t, shape)
    square = t * t
    row = rows_of(shape)
    pair = jnp.minimum(row, 7 - row)
    point, scale = F32(NODE_POINTS[7]), F32(NODE_SCALE[7])
    for a in range(7):
        point = jnp.where(row == a, F32(NODE_POINTS[a]), point)
        scale = jnp.where(row == a, F32(NODE_SCALE[a]), scale)
    own = (t + point) * scale
    out = None
    for m in range(4):
        factor = jnp.where(pair == m, own, square - F32(NODE_POINTS[m] ** 2))
        out = factor if out is None else out * factor
    return out


def move(x, k):
    return pltpu.roll(x, k % x.shape[1], 1)


def exchange_kernel(
    n_grp, n_dev, coord, resid, weight, dest, slot, elem, mid, cost,
    coord_v, resid_v, weight_v, dest_v, slot_v, elem_v,
    lhs, pick, send, recv, acc, outer, summed, bases, xo, xi, oh,
    c1s, c1r, c2s, c2r, halo_g, halo_d, halo_c, gsend, dsend,
    in_sem, send_sem, recv_sem, c1_ssem, c1_rsem, c2_ssem, c2_rsem, h_ssem, h_rsem,
):
    g, d = lax.axis_index("grp"), lax.axis_index("dev")
    co = min(COPLANE, n_dev)
    planes = n_dev // co
    steps = peer_steps(n_dev)
    here = lax.rem(d, co)
    block = d - here
    y, z, core = d // co, here // 2, lax.rem(d, 2)
    to_y = [lax.rem(y + k, planes) * co for k in range(planes)]
    to_z = [lax.rem(z + k, co // 2) * 2 for k in range(co // 2)]
    to_core = [core, 1 - core]
    peer_at = [to_y[i] + to_z[j] + to_core[k] for i, j, k in steps]

    def at(dg, dd):
        return {"grp": lax.rem(g + dg + n_grp, n_grp), "dev": lax.rem(d + dd + n_dev, n_dev)}

    loads = [
        pltpu.make_async_copy(src, dst, in_sem.at[i])
        for i, (src, dst) in enumerate(
            [(dest, dest_v), (slot, slot_v), (elem, elem_v), (coord, coord_v), (resid, resid_v), (weight, weight_v)]
        )
    ]
    barrier = pltpu.get_barrier_semaphore()
    corners = [(-1, -1), (-1, 1), (1, -1), (1, 1)]
    peers = [(k, p * co) for k in range(1, n_grp) for p in range(planes)]
    peers += corners
    targets = [{"grp": g, "dev": peer} for peer in reversed(peer_at[1:])]
    targets += [at(dg, dd) for dg, dd in peers]
    for i, target in enumerate(targets):
        if i == len(targets) // 2:
            for load in loads:
                load.start()
        pl.semaphore_signal(barrier, inc=1, device_id=target)
    for load in loads:
        load.wait()

    for j in range(resid_v.shape[0] // 2):
        def pair(ref):
            return jnp.concatenate([ref[2 * j : 2 * j + 1, :], ref[2 * j + 1 : 2 * j + 2, :]], axis=1)

        cols = slice(256 * j, 256 * j + 256)
        to = pair(dest_v)
        upper = to >> 5
        mask = one_hot((to - 32 * upper).astype(F32), 32)
        pick[:, cols] = one_hot((upper * CAP + pair(slot_v)).astype(F32), 256)
        parts = []
        for value in [coord_v[c : c + 1, cols] for c in range(3)] + [pair(weight_v) * pair(resid_v)]:
            high = high_of(value)
            parts += [high, value - high]
        parts.append(pair(elem_v).astype(F32))
        for i, part in enumerate(parts):
            wide = jnp.broadcast_to(part, (16, 256)).astype(BF16)
            lhs[32 * i : 32 * i + 32, cols] = mask * jnp.concatenate([wide, wide], axis=0)
    packed = lax.dot_general(lhs[...], pick[...], NT, preferred_element_type=F32)
    part = [packed[32 * k : 32 * k + 32] for k in range(9)]
    values = [part[2 * c] + part[2 * c + 1] for c in range(4)] + [part[8]]
    for c, value in enumerate(values):
        send[0:32, c, :] = value[:, :CAP]
        send[32:64, c, :] = value[:, CAP:]
    r = resid_v[...]
    c1s[...] = jnp.sum(weight_v[...] * r * r, axis=0, keepdims=True)

    recv[0] = send[d]
    c1r[here] = c1s[...]

    pl.semaphore_wait(barrier, len(targets))

    bounds = bounds_of(n_dev)
    chunks = list(zip(bounds[:-1], bounds[1:]))
    chunk_of = [i for i, (first, last) in enumerate(chunks) for _ in range(first, last)]

    def message(k):
        to = peer_at[k]
        return pltpu.make_async_remote_copy(
            src_ref=send.at[to],
            dst_ref=recv.at[k],
            send_sem=send_sem,
            recv_sem=recv_sem.at[chunk_of[k]],
            device_id={"grp": g, "dev": to},
        )

    def await_bytes(ref, sem):
        pltpu.make_async_copy(ref, ref, sem).wait()

    def partial_one(k):
        return pltpu.make_async_remote_copy(
            src_ref=c1s, dst_ref=c1r.at[here], send_sem=c1_ssem, recv_sem=c1_rsem,
            device_id={"grp": g, "dev": block + lax.rem(here + k, co)},
        )

    for k in range(1, co):
        partial_one(k).start()
    for k in range(1, n_dev):
        message(k).start()

    mine = g * planes + block // co
    rest = [(k, p) for k in range(n_grp) for p in range(planes) if k or p]
    twos = [
        pltpu.make_async_remote_copy(
            src_ref=c2s, dst_ref=c2r.at[mine], send_sem=c2_ssem, recv_sem=c2_rsem,
            device_id=at(k, p * co),
        )
        for k, p in rest
    ]

    def rows_built(ref, cols, groups, fa, fb, fc):
        bc = [fb[b : b + 1] * fc for b in range(8)]
        count = 8 * len(groups)
        for k in range(0, len(groups), 2):
            full = jnp.concatenate([fa[a : a + 1] * bc[b] for a, b in groups[k : k + 2]], axis=0)
            high = full.astype(BF16)
            low = (full - high.astype(F32)).astype(BF16)
            ref[8 * k : 8 * k + 16, cols] = high
            ref[count + 8 * k : count + 8 * k + 16, cols] = low

    def cols_of(i, p):
        begin = 256 * p - CAP * chunks[i][0]
        return slice(begin, begin + 256)

    def build(i, p):
        first, second = recv[2 * p], recv[2 * p + 1]

        def row(c):
            return jnp.concatenate([first[c : c + 1], second[c : c + 1]], axis=1)

        cols = cols_of(i, p)
        fa = basis(row(0)) * row(3)
        fb = basis(row(1))
        fc = basis(row(2))
        for c, value in enumerate((fa, fb, fc)):
            bases[c, p] = value
        rows_built(xo[i], cols, OUTER, fa, fb, fc)
        oh[i][:, cols] = one_hot(row(4), ELEM)

    def product(ref, i):
        return lax.dot_general(ref[i][...], oh[i][...], NT, preferred_element_type=F32)

    def arrived(i):
        first, last = max(chunks[i][0], 1), chunks[i][1]
        await_bytes(recv.at[first:last], recv_sem.at[i])

    def block_of(body):
        pl.when(d >= 0)(body)

    for i in range(len(chunks)):
        arrived(i)

        @block_of
        def _():
            for p in range(chunks[i][0] // 2, chunks[i][1] // 2):
                build(i, p)
            now = product(xo, i)
            if i > 0:
                now = acc[...] + now
            if i + 1 < len(chunks):
                acc[...] = now
            else:
                outer[...] = now[:SPLIT] + now[SPLIT:]

        if i == 1:
            await_bytes(c1r.at[1:co], c1_rsem)
            total = c1r[0]
            for k in range(1, co):
                total += c1r[k]
            c2s[...] = total
            c2r[mine] = total
            for m in twos:
                m.start()

    def exists(dg, dd):
        return (g + dg >= 0) & (g + dg < n_grp) & (d + dd >= 0) & (d + dd < n_dev)

    halo_steps = [(-1, 0), (1, 0), (0, -1), (0, 1)] + corners
    halo_slots = [halo_g.at[0], halo_g.at[1], halo_d.at[0], halo_d.at[1]]
    halo_slots += [halo_c.at[i] for i in range(4)]

    def halo(i, src):
        dg, dd = halo_steps[i]

        @pl.when(exists(dg, dd))
        def _():
            pltpu.make_async_remote_copy(
                src_ref=src, dst_ref=halo_slots[i], send_sem=h_ssem.at[i], recv_sem=h_rsem.at[i],
                device_id=at(dg, dd),
            ).start()

    def line(a, b):
        first, half = PLACE[a, b], 128 if a else 0
        return outer.at[first : first + 8, half : half + 128]

    for i, (dg, dd) in enumerate(corners):
        halo(4 + i, line(0 if dg < 0 else 7, 0 if dd < 0 else 7))

    lane = lanes_of((8, ELEM))
    half = lanes_of((8, 128))

    def rg(ref, a, b):
        return ref[PLACE[a, b] : PLACE[a, b] + 8, :]

    def put(ref, a, b, value):
        ref[PLACE[a, b] : PLACE[a, b] + 8, :] = value

    now = {ab: rg(outer, *ab) for ab in OUTER}
    for b in (0, 7, 1, 2, 3, 4, 5, 6):
        low, high = now[0, b], now[7, b]
        now[0, b] = low + jnp.where(lane >= 64, move(high, 64), 0.0)
        now[7, b] = high + jnp.where(lane < 192, move(low, -64), 0.0)
        put(summed, 0, b, now[0, b])
        put(summed, 7, b, now[7, b])
    for side, b, step in ((0, 0, 8), (1, 7, -8)):
        near = ((half >> 3) & 7) == b
        for first in (0, 4):
            packed_planes = None
            for j in range(4):
                plane = now[first + j, b]
                left = jnp.where(near, plane[:, :128], 0.0)
                right = jnp.where(near, plane[:, 128:], 0.0)
                piece = move(left + move(right, step), 2 * step * j)
                packed_planes = piece if j == 0 else packed_planes + piece
            dsend[side, 2 * first : 2 * first + 8, :] = packed_planes
    for side in range(2):
        halo(2 + side, dsend.at[side])
    for b in range(4):
        gsend[0, 8 * b : 8 * b + 8, :] = jnp.where(
            half < 64, rg(outer, 0, b)[:, :128], move(rg(outer, 0, b + 4)[:, :128], 64)
        )
        gsend[1, 8 * b : 8 * b + 8, :] = jnp.where(
            half < 64, move(rg(outer, 7, b)[:, 128:], 64), rg(outer, 7, b + 4)[:, 128:]
        )
    for side in range(2):
        halo(side, gsend.at[side])

    @block_of
    def _():
        left = None
        for i, (first, last) in enumerate(chunks):
            for p in range(first // 2, last // 2):
                rows_built(xi[i], cols_of(i, p), INNER, *[bases[c, p] for c in range(3)])
            now = product(xi, i)
            left = now if left is None else left + now
        mid[SPLIT:, :] = left[: NODES - SPLIT] + left[NODES - SPLIT :]


    for i, (dg, dd) in enumerate(halo_steps):

        @pl.when(exists(-dg, -dd))
        def _():
            await_bytes(halo_slots[i], h_rsem.at[i])


    up_g, down_g = g > 0, g < n_grp - 1
    up_d, down_d = d > 0, d < n_dev - 1
    ey = (lane >> 3) & 7

    def wide(value):
        return jnp.concatenate([value, value], axis=1)

    planes_now = {(a, b): rg(summed if a in EDGE else outer, a, b) for a, b in OUTER}
    for b in range(8):
        part = slice(8 * (b % 4), 8 * (b % 4) + 8)
        from_low, from_high = halo_g[1, part, :], halo_g[0, part, :]
        if b < 4:
            from_high = move(from_high, 64)
        else:
            from_low = move(from_low, 64)
        planes_now[0, b] += jnp.where((lane < 64) & up_g, wide(from_low), 0.0)
        planes_now[7, b] += jnp.where((lane >= 192) & down_g, wide(from_high), 0.0)
    for a in range(8):
        low, high = planes_now[a, 0], planes_now[a, 7]
        part, shift = slice(8 * (a // 4), 8 * (a // 4) + 8), 16 * (a % 4)
        theirs = halo_d[1, part, :]
        to_low = jnp.concatenate([move(theirs, shift - 56), move(theirs, shift - 48)], axis=1)
        theirs = halo_d[0, part, :]
        to_high = jnp.concatenate([move(theirs, 56 - shift), move(theirs, 48 - shift)], axis=1)
        if a == 0:
            to_low += jnp.where((lane < 8) & up_g, wide(move(halo_c[3], -120)), 0.0)
            to_high += jnp.where((lane >= 56) & (lane < 64) & up_g, wide(move(halo_c[2], -8)), 0.0)
        if a == 7:
            to_low += jnp.where((lane >= 192) & (lane < 200) & down_g, wide(move(halo_c[1], 8)), 0.0)
            to_high += jnp.where((lane >= 248) & down_g, wide(move(halo_c[0], 120)), 0.0)
        new_low = jnp.where(ey > 0, move(high, 8), jnp.where(up_d, to_low, 0.0))
        new_high = jnp.where(ey < 7, move(low, -8), jnp.where(down_d, to_high, 0.0))
        planes_now[a, 0] = low + new_low
        planes_now[a, 7] = high + new_high
    for ab in OUTER:
        put(mid, *ab, planes_now[ab])

    await_bytes(c2r.at[1:], c2_rsem)
    total = c2r[0]
    for k in range(1, n_grp * planes):
        total += c2r[k]
    cost[...] = total
    await_bytes(recv.at[1:], send_sem)
    await_bytes(c1r.at[1:], c1_ssem)
    await_bytes(c2r.at[1:], c2_ssem)
    for i, (dg, dd) in enumerate(halo_steps):

        @pl.when(exists(dg, dd))
        def _():
            await_bytes(halo_slots[i], h_ssem.at[i])


def finish_kernel(mid, cost_row, out, cost):
    shape = (8, 128)
    ez = lanes_of(shape) & 7
    row = rows_of(shape)
    done = {}
    for ab in GROUPS:
        now = mid[PLACE[ab] : PLACE[ab] + 8, :]
        z = jnp.where(row == 7, move(now, 1), move(now, -1))
        to_low = jnp.where((row == 0) & (ez > 0), pltpu.roll(z, 1, 0), 0.0)
        to_high = jnp.where((row == 7) & (ez < 7), pltpu.roll(z, 7, 0), 0.0)
        done[ab] = now + to_low + to_high
    for a in range(0, 8, 2):
        both = jnp.concatenate([done[k, b] for k in (a, a + 1) for b in range(8)], axis=0)
        out[:, 64 * a : 64 * a + 128] = both.T
    cost[0, 0] = 0.5 * jnp.sum(cost_row[...])


def on_device(coord, resid, weight, dest, slot, elem, n_grp, n_dev):
    rows = resid.shape[0] // 128
    flat = [v.reshape(rows, 128) for v in (resid, weight, dest, slot, elem)]
    co = min(COPLANE, n_dev)
    blocks = n_grp * (n_dev // co)
    dma = pltpu.SemaphoreType.DMA
    bounds = bounds_of(n_dev)
    widths = [CAP * (last - first) for first, last in zip(bounds[:-1], bounds[1:])]
    vmem = pl.BlockSpec(memory_space=pltpu.VMEM)
    mid, cost_row = pl.pallas_call(
        functools.partial(exchange_kernel, n_grp, n_dev),
        out_shape=(
            jax.ShapeDtypeStruct((NODES, ELEM), F32),
            jax.ShapeDtypeStruct((1, 128), F32),
        ),
        in_specs=[pl.BlockSpec(memory_space=pltpu.HBM)] * 6,
        out_specs=(vmem, vmem),
        scratch_shapes=[
            pltpu.VMEM(coord.shape, F32),
            pltpu.VMEM((rows, 128), F32),
            pltpu.VMEM((rows, 128), F32),
            pltpu.VMEM((rows, 128), I32),
            pltpu.VMEM((rows, 128), I32),
            pltpu.VMEM((rows, 128), I32),
            pltpu.VMEM((9 * 32, rows * 128), BF16),
            pltpu.VMEM((256, rows * 128), BF16),
            pltpu.VMEM((PEERS, 5, CAP), F32),
            pltpu.VMEM((n_dev, 5, CAP), F32),
            pltpu.VMEM((2 * SPLIT, ELEM), F32),
            pltpu.VMEM((SPLIT, ELEM), F32),
            pltpu.VMEM((128, ELEM), F32),
            pltpu.VMEM((3, n_dev // 2, 8, 256), F32),
            [pltpu.VMEM((2 * SPLIT, n), BF16) for n in widths],
            [pltpu.VMEM((2 * (NODES - SPLIT), n), BF16) for n in widths],
            [pltpu.VMEM((ELEM, n), BF16) for n in widths],
            pltpu.VMEM((1, 128), F32),
            pltpu.VMEM((co, 1, 128), F32),
            pltpu.VMEM((1, 128), F32),
            pltpu.VMEM((blocks, 1, 128), F32),
            pltpu.VMEM((2, 32, 128), F32),
            pltpu.VMEM((2, 16, 128), F32),
            pltpu.VMEM((4, 8, 128), F32),
            pltpu.VMEM((2, 32, 128), F32),
            pltpu.VMEM((2, 16, 128), F32),
            dma((6,)),
            dma,
            dma((len(widths),)),
            dma,
            dma,
            dma,
            dma,
            dma((8,)),
            dma((8,)),
        ],
        compiler_params=pltpu.CompilerParams(
            collective_id=0, has_side_effects=True, vmem_limit_bytes=48 * 1024 * 1024
        ),
    )(*[pltpu.with_memory_space_constraint(v, pltpu.HBM) for v in (coord, *flat)])
    out, cost = pl.pallas_call(
        finish_kernel,
        grid=(ELEM // 128,),
        out_shape=(
            jax.ShapeDtypeStruct((ELEM, NODES), F32),
            jax.ShapeDtypeStruct((1, 1), F32),
        ),
        in_specs=[
            pl.BlockSpec((NODES, 128), lambda i: (0, i)),
            pl.BlockSpec((1, 128), lambda i: (0, 0)),
        ],
        out_specs=(
            pl.BlockSpec((128, NODES), lambda i: (i, 0)),
            pl.BlockSpec(memory_space=pltpu.SMEM),
        ),
        compiler_params=pltpu.CompilerParams(vmem_limit_bytes=16 * 1024 * 1024),
    )(mid, cost_row)
    return out.reshape(4, 8, 8, NODES), cost.reshape(())


def solution(mesh):
    n_grp, n_dev = mesh.shape["grp"], mesh.shape["dev"]
    rows = P(("grp", "dev"))

    def step(obs_coord, obs_resid, obs_weight, obs_dest, obs_send_slot, obs_elem, obs_slot):
        del obs_slot
        return on_device(
            obs_coord, obs_resid, obs_weight, obs_dest, obs_send_slot, obs_elem, n_grp, n_dev
        )

    return jax.shard_map(
        step,
        mesh=mesh,
        in_specs=(P(None, ("grp", "dev")), rows, rows, rows, rows, rows, rows),
        out_specs=(P("grp", "dev", None, None), P()),
        check_vma=False,
    )
```

```python
import functools
import math

import jax
import jax.numpy as jnp
from jax import lax
from jax.experimental import pallas as pl
from jax.experimental.pallas import tpu as pltpu
from jax.sharding import PartitionSpec as P

CAP = 128
ELEM = 256
NODES = 512
COPLANE = 16
PEERS = 64
NODE_POINTS = [-math.cos(math.pi * k / 7) for k in range(8)]
NODE_SCALE = [
    1.0 / math.prod(NODE_POINTS[a] - NODE_POINTS[m] for m in range(8) if m != a)
    for a in range(8)
]
NT = (((1,), (1,)), ((), ()))
F32, BF16, I32 = jnp.float32, jnp.bfloat16, jnp.int32
EDGE = (0, 7)
OUTER = [(a, b) for a in range(8) for b in range(8) if a in EDGE or b in EDGE]
INNER = [(a, b) for a in range(8) for b in range(8) if not (a in EDGE or b in EDGE)]
OUTER.sort(key=lambda ab: (EDGE.index(ab[0]) if ab[0] in EDGE else 2, ab))
GROUPS = OUTER + INNER
PLACE = {ab: 8 * i for i, ab in enumerate(GROUPS)}
SPLIT = 8 * len(OUTER)


def peer_steps(n_dev):
    size_y, size_z = n_dev // min(COPLANE, n_dev), min(COPLANE, n_dev) // 2
    steps = [(y, z, c) for y in range(size_y) for z in range(size_z) for c in range(2)]

    def hops(step):
        y, z, _ = step
        return min(y, size_y - y) + min(z, size_z - z)

    return sorted(steps, key=lambda step: (hops(step), step))


def bounds_of(n_dev):
    return [0, 8, 24, 40, 52, 64] if n_dev == 64 else [0, 2, 4]


def lanes_of(shape):
    return lax.broadcasted_iota(I32, shape, len(shape) - 1)


def rows_of(shape):
    return lax.broadcasted_iota(I32, shape, len(shape) - 2)


def high_of(value):
    return value.astype(BF16).astype(F32)


def one_hot(ids, count):
    shape = (count, ids.shape[1])
    ids = jnp.broadcast_to(ids, (16, ids.shape[1])).astype(BF16)
    ids = jnp.concatenate([ids] * (count // 16), axis=0)
    row = rows_of(shape).astype(F32).astype(BF16)
    return jnp.where(row == ids, jnp.ones(shape, BF16), jnp.zeros(shape, BF16))


def basis(t):
    shape = (8, t.shape[1])
    t = jnp.broadcast_to(t, shape)
    square = t * t
    row = rows_of(shape)
    pair = jnp.minimum(row, 7 - row)
    point, scale = F32(NODE_POINTS[7]), F32(NODE_SCALE[7])
    for a in range(7):
        point = jnp.where(row == a, F32(NODE_POINTS[a]), point)
        scale = jnp.where(row == a, F32(NODE_SCALE[a]), scale)
    own = (t + point) * scale
    out = None
    for m in range(4):
        factor = jnp.where(pair == m, own, square - F32(NODE_POINTS[m] ** 2))
        out = factor if out is None else out * factor
    return out


def move(x, k):
    return pltpu.roll(x, k % x.shape[1], 1)


def exchange_kernel(
    n_grp, n_dev, coord, resid, weight, dest, slot, elem, mid, cost,
    coord_v, resid_v, weight_v, dest_v, slot_v, elem_v,
    lhs, pick, send, recv, acc, outer, summed, bases, xo, xi, oh,
    c1s, c1r, c2s, c2r, halo_g, halo_d, halo_c, gsend, dsend,
    in_sem, send_sem, recv_sem, c1_ssem, c1_rsem, c2_ssem, c2_rsem, h_ssem, h_rsem,
):
    g, d = lax.axis_index("grp"), lax.axis_index("dev")
    co = min(COPLANE, n_dev)
    planes = n_dev // co
    steps = peer_steps(n_dev)
    here = lax.rem(d, co)
    block = d - here
    y, z, core = d // co, here // 2, lax.rem(d, 2)
    to_y = [lax.rem(y + k, planes) * co for k in range(planes)]
    to_z = [lax.rem(z + k, co // 2) * 2 for k in range(co // 2)]
    to_core = [core, 1 - core]
    peer_at = [to_y[i] + to_z[j] + to_core[k] for i, j, k in steps]

    def at(dg, dd):
        return {"grp": lax.rem(g + dg + n_grp, n_grp), "dev": lax.rem(d + dd + n_dev, n_dev)}

    loads = [
        pltpu.make_async_copy(src, dst, in_sem.at[i])
        for i, (src, dst) in enumerate(
            [(dest, dest_v), (slot, slot_v), (elem, elem_v), (coord, coord_v), (resid, resid_v), (weight, weight_v)]
        )
    ]
    barrier = pltpu.get_barrier_semaphore()
    corners = [(-1, -1), (-1, 1), (1, -1), (1, 1)]
    peers = [(k, p * co) for k in range(1, n_grp) for p in range(planes)]
    peers += corners
    targets = [{"grp": g, "dev": peer} for peer in reversed(peer_at[1:])]
    targets += [at(dg, dd) for dg, dd in peers]
    for i, target in enumerate(targets):
        if i == len(targets) // 2:
            for load in loads:
                load.start()
        pl.semaphore_signal(barrier, inc=1, device_id=target)
    for load in loads:
        load.wait()

    for j in range(resid_v.shape[0] // 2):
        def pair(ref):
            return jnp.concatenate([ref[2 * j : 2 * j + 1, :], ref[2 * j + 1 : 2 * j + 2, :]], axis=1)

        cols = slice(256 * j, 256 * j + 256)
        to = pair(dest_v)
        upper = to >> 5
        mask = one_hot((to - 32 * upper).astype(F32), 32)
        pick[:, cols] = one_hot((upper * CAP + pair(slot_v)).astype(F32), 256)
        parts = []
        for value in [coord_v[c : c + 1, cols] for c in range(3)] + [pair(weight_v) * pair(resid_v)]:
            high = high_of(value)
            parts += [high, value - high]
        parts.append(pair(elem_v).astype(F32))
        for i, part in enumerate(parts):
            wide = jnp.broadcast_to(part, (16, 256)).astype(BF16)
            lhs[32 * i : 32 * i + 32, cols] = mask * jnp.concatenate([wide, wide], axis=0)
    packed = lax.dot_general(lhs[...], pick[...], NT, preferred_element_type=F32)
    part = [packed[32 * k : 32 * k + 32] for k in range(9)]
    values = [part[2 * c] + part[2 * c + 1] for c in range(4)] + [part[8]]
    for c, value in enumerate(values):
        send[0:32, c, :] = value[:, :CAP]
        send[32:64, c, :] = value[:, CAP:]
    r = resid_v[...]
    c1s[...] = jnp.sum(weight_v[...] * r * r, axis=0, keepdims=True)

    recv[0] = send[d]
    c1r[here] = c1s[...]

    pl.semaphore_wait(barrier, len(targets))

    bounds = bounds_of(n_dev)
    chunks = list(zip(bounds[:-1], bounds[1:]))
    chunk_of = [i for i, (first, last) in enumerate(chunks) for _ in range(first, last)]

    def message(k):
        to = peer_at[k]
        return pltpu.make_async_remote_copy(
            src_ref=send.at[to],
            dst_ref=recv.at[k],
            send_sem=send_sem,
            recv_sem=recv_sem.at[chunk_of[k]],
            device_id={"grp": g, "dev": to},
        )

    def await_bytes(ref, sem):
        pltpu.make_async_copy(ref, ref, sem).wait()

    def partial_one(k):
        return pltpu.make_async_remote_copy(
            src_ref=c1s, dst_ref=c1r.at[here], send_sem=c1_ssem, recv_sem=c1_rsem,
            device_id={"grp": g, "dev": block + lax.rem(here + k, co)},
        )

    for k in range(1, n_dev):
        message(k).start()
        if k == n_dev // 4:
            for j in range(1, co):
                partial_one(j).start()

    mine = g * planes + block // co
    rest = [(k, p) for k in range(n_grp) for p in range(planes) if k or p]
    twos = [
        pltpu.make_async_remote_copy(
            src_ref=c2s, dst_ref=c2r.at[mine], send_sem=c2_ssem, recv_sem=c2_rsem,
            device_id=at(k, p * co),
        )
        for k, p in rest
    ]

    def rows_built(ref, cols, groups, fa, fb, fc):
        bc = [fb[b : b + 1] * fc for b in range(8)]
        count = 8 * len(groups)
        for k in range(0, len(groups), 2):
            full = jnp.concatenate([fa[a : a + 1] * bc[b] for a, b in groups[k : k + 2]], axis=0)
            high = full.astype(BF16)
            low = (full - high.astype(F32)).astype(BF16)
            ref[8 * k : 8 * k + 16, cols] = high
            ref[count + 8 * k : count + 8 * k + 16, cols] = low

    def cols_of(i, p):
        begin = 256 * p - CAP * chunks[i][0]
        return slice(begin, begin + 256)

    def build(i, p):
        first, second = recv[2 * p], recv[2 * p + 1]

        def row(c):
            return jnp.concatenate([first[c : c + 1], second[c : c + 1]], axis=1)

        cols = cols_of(i, p)
        fa = basis(row(0)) * row(3)
        fb = basis(row(1))
        fc = basis(row(2))
        for c, value in enumerate((fa, fb, fc)):
            bases[c, p] = value
        rows_built(xo[i], cols, OUTER, fa, fb, fc)
        oh[i][:, cols] = one_hot(row(4), ELEM)

    def product(ref, i):
        return lax.dot_general(ref[i][...], oh[i][...], NT, preferred_element_type=F32)

    def arrived(i):
        first, last = max(chunks[i][0], 1), chunks[i][1]
        await_bytes(recv.at[first:last], recv_sem.at[i])

    def block_of(body):
        pl.when(d >= 0)(body)

    for i in range(len(chunks)):
        arrived(i)

        def contract():
            for p in range(chunks[i][0] // 2, chunks[i][1] // 2):
                build(i, p)
            now = product(xo, i)
            if i > 0:
                now = acc[...] + now
            if i + 1 < len(chunks):
                acc[...] = now
            else:
                outer[...] = now[:SPLIT] + now[SPLIT:]

        if i + 1 < len(chunks):
            block_of(contract)
        else:
            contract()

        if i == 1:
            await_bytes(c1r.at[1:co], c1_rsem)
            total = c1r[0]
            for k in range(1, co):
                total += c1r[k]
            c2s[...] = total
            c2r[mine] = total
            for m in twos:
                m.start()

    def exists(dg, dd):
        return (g + dg >= 0) & (g + dg < n_grp) & (d + dd >= 0) & (d + dd < n_dev)

    halo_steps = [(-1, 0), (1, 0), (0, -1), (0, 1)] + corners
    halo_slots = [halo_g.at[0], halo_g.at[1], halo_d.at[0], halo_d.at[1]]
    halo_slots += [halo_c.at[i] for i in range(4)]

    def halo(i, src):
        dg, dd = halo_steps[i]

        @pl.when(exists(dg, dd))
        def _():
            pltpu.make_async_remote_copy(
                src_ref=src, dst_ref=halo_slots[i], send_sem=h_ssem.at[i], recv_sem=h_rsem.at[i],
                device_id=at(dg, dd),
            ).start()

    def line(a, b):
        first, half = PLACE[a, b], 128 if a else 0
        return outer.at[first : first + 8, half : half + 128]

    for i, (dg, dd) in enumerate(corners):
        halo(4 + i, line(0 if dg < 0 else 7, 0 if dd < 0 else 7))

    lane = lanes_of((8, ELEM))
    half = lanes_of((8, 128))

    def rg(ref, a, b):
        return ref[PLACE[a, b] : PLACE[a, b] + 8, :]

    def put(ref, a, b, value):
        ref[PLACE[a, b] : PLACE[a, b] + 8, :] = value

    now = {ab: rg(outer, *ab) for ab in OUTER}
    for b in (0, 7, 1, 2, 3, 4, 5, 6):
        low, high = now[0, b], now[7, b]
        now[0, b] = low + jnp.where(lane >= 64, move(high, 64), 0.0)
        now[7, b] = high + jnp.where(lane < 192, move(low, -64), 0.0)
        put(summed, 0, b, now[0, b])
        put(summed, 7, b, now[7, b])
    for side, b, step in ((0, 0, 8), (1, 7, -8)):
        near = ((half >> 3) & 7) == b
        for first in (0, 4):
            packed_planes = None
            for j in range(4):
                plane = now[first + j, b]
                left = jnp.where(near, plane[:, :128], 0.0)
                right = jnp.where(near, plane[:, 128:], 0.0)
                piece = move(left + move(right, step), 2 * step * j)
                packed_planes = piece if j == 0 else packed_planes + piece
            dsend[side, 2 * first : 2 * first + 8, :] = packed_planes
    for side in range(2):
        halo(2 + side, dsend.at[side])
    for b in range(4):
        gsend[0, 8 * b : 8 * b + 8, :] = jnp.where(
            half < 64, rg(outer, 0, b)[:, :128], move(rg(outer, 0, b + 4)[:, :128], 64)
        )
        gsend[1, 8 * b : 8 * b + 8, :] = jnp.where(
            half < 64, move(rg(outer, 7, b)[:, 128:], 64), rg(outer, 7, b + 4)[:, 128:]
        )
    for side in range(2):
        halo(side, gsend.at[side])

    @block_of
    def _():
        left = None
        for i, (first, last) in enumerate(chunks):
            for p in range(first // 2, last // 2):
                rows_built(xi[i], cols_of(i, p), INNER, *[bases[c, p] for c in range(3)])
            now = product(xi, i)
            left = now if left is None else left + now
        mid[SPLIT:, :] = left[: NODES - SPLIT] + left[NODES - SPLIT :]


    for i, (dg, dd) in enumerate(halo_steps):

        @pl.when(exists(-dg, -dd))
        def _():
            await_bytes(halo_slots[i], h_rsem.at[i])


    up_g, down_g = g > 0, g < n_grp - 1
    up_d, down_d = d > 0, d < n_dev - 1
    ey = (lane >> 3) & 7

    def wide(value):
        return jnp.concatenate([value, value], axis=1)

    planes_now = {(a, b): rg(summed if a in EDGE else outer, a, b) for a, b in OUTER}
    for b in range(8):
        part = slice(8 * (b % 4), 8 * (b % 4) + 8)
        from_low, from_high = halo_g[1, part, :], halo_g[0, part, :]
        if b < 4:
            from_high = move(from_high, 64)
        else:
            from_low = move(from_low, 64)
        planes_now[0, b] += jnp.where((lane < 64) & up_g, wide(from_low), 0.0)
        planes_now[7, b] += jnp.where((lane >= 192) & down_g, wide(from_high), 0.0)
    for a in range(8):
        low, high = planes_now[a, 0], planes_now[a, 7]
        part, shift = slice(8 * (a // 4), 8 * (a // 4) + 8), 16 * (a % 4)
        theirs = halo_d[1, part, :]
        to_low = jnp.concatenate([move(theirs, shift - 56), move(theirs, shift - 48)], axis=1)
        theirs = halo_d[0, part, :]
        to_high = jnp.concatenate([move(theirs, 56 - shift), move(theirs, 48 - shift)], axis=1)
        if a == 0:
            to_low += jnp.where((lane < 8) & up_g, wide(move(halo_c[3], -120)), 0.0)
            to_high += jnp.where((lane >= 56) & (lane < 64) & up_g, wide(move(halo_c[2], -8)), 0.0)
        if a == 7:
            to_low += jnp.where((lane >= 192) & (lane < 200) & down_g, wide(move(halo_c[1], 8)), 0.0)
            to_high += jnp.where((lane >= 248) & down_g, wide(move(halo_c[0], 120)), 0.0)
        new_low = jnp.where(ey > 0, move(high, 8), jnp.where(up_d, to_low, 0.0))
        new_high = jnp.where(ey < 7, move(low, -8), jnp.where(down_d, to_high, 0.0))
        planes_now[a, 0] = low + new_low
        planes_now[a, 7] = high + new_high
    for ab in OUTER:
        put(mid, *ab, planes_now[ab])

    await_bytes(c2r.at[1:], c2_rsem)
    total = c2r[0]
    for k in range(1, n_grp * planes):
        total += c2r[k]
    cost[...] = total
    await_bytes(recv.at[1:], send_sem)
    await_bytes(c1r.at[1:], c1_ssem)
    await_bytes(c2r.at[1:], c2_ssem)
    for i, (dg, dd) in enumerate(halo_steps):

        @pl.when(exists(dg, dd))
        def _():
            await_bytes(halo_slots[i], h_ssem.at[i])


def finish_kernel(mid, cost_row, out, cost):
    shape = (8, 128)
    ez = lanes_of(shape) & 7
    row = rows_of(shape)
    done = {}
    for ab in GROUPS:
        now = mid[PLACE[ab] : PLACE[ab] + 8, :]
        z = jnp.where(row == 7, move(now, 1), move(now, -1))
        to_low = jnp.where((row == 0) & (ez > 0), pltpu.roll(z, 1, 0), 0.0)
        to_high = jnp.where((row == 7) & (ez < 7), pltpu.roll(z, 7, 0), 0.0)
        done[ab] = now + to_low + to_high
    for a in range(0, 8, 2):
        both = jnp.concatenate([done[k, b] for k in (a, a + 1) for b in range(8)], axis=0)
        out[:, 64 * a : 64 * a + 128] = both.T
    cost[0, 0] = 0.5 * jnp.sum(cost_row[...])


def on_device(coord, resid, weight, dest, slot, elem, n_grp, n_dev):
    rows = resid.shape[0] // 128
    flat = [v.reshape(rows, 128) for v in (resid, weight, dest, slot, elem)]
    co = min(COPLANE, n_dev)
    blocks = n_grp * (n_dev // co)
    dma = pltpu.SemaphoreType.DMA
    bounds = bounds_of(n_dev)
    widths = [CAP * (last - first) for first, last in zip(bounds[:-1], bounds[1:])]
    vmem = pl.BlockSpec(memory_space=pltpu.VMEM)
    mid, cost_row = pl.pallas_call(
        functools.partial(exchange_kernel, n_grp, n_dev),
        out_shape=(
            jax.ShapeDtypeStruct((NODES, ELEM), F32),
            jax.ShapeDtypeStruct((1, 128), F32),
        ),
        in_specs=[pl.BlockSpec(memory_space=pltpu.HBM)] * 6,
        out_specs=(vmem, vmem),
        scratch_shapes=[
            pltpu.VMEM(coord.shape, F32),
            pltpu.VMEM((rows, 128), F32),
            pltpu.VMEM((rows, 128), F32),
            pltpu.VMEM((rows, 128), I32),
            pltpu.VMEM((rows, 128), I32),
            pltpu.VMEM((rows, 128), I32),
            pltpu.VMEM((9 * 32, rows * 128), BF16),
            pltpu.VMEM((256, rows * 128), BF16),
            pltpu.VMEM((PEERS, 5, CAP), F32),
            pltpu.VMEM((n_dev, 5, CAP), F32),
            pltpu.VMEM((2 * SPLIT, ELEM), F32),
            pltpu.VMEM((SPLIT, ELEM), F32),
            pltpu.VMEM((128, ELEM), F32),
            pltpu.VMEM((3, n_dev // 2, 8, 256), F32),
            [pltpu.VMEM((2 * SPLIT, n), BF16) for n in widths],
            [pltpu.VMEM((2 * (NODES - SPLIT), n), BF16) for n in widths],
            [pltpu.VMEM((ELEM, n), BF16) for n in widths],
            pltpu.VMEM((1, 128), F32),
            pltpu.VMEM((co, 1, 128), F32),
            pltpu.VMEM((1, 128), F32),
            pltpu.VMEM((blocks, 1, 128), F32),
            pltpu.VMEM((2, 32, 128), F32),
            pltpu.VMEM((2, 16, 128), F32),
            pltpu.VMEM((4, 8, 128), F32),
            pltpu.VMEM((2, 32, 128), F32),
            pltpu.VMEM((2, 16, 128), F32),
            dma((6,)),
            dma,
            dma((len(widths),)),
            dma,
            dma,
            dma,
            dma,
            dma((8,)),
            dma((8,)),
        ],
        compiler_params=pltpu.CompilerParams(
            collective_id=0, has_side_effects=True, vmem_limit_bytes=48 * 1024 * 1024
        ),
    )(*[pltpu.with_memory_space_constraint(v, pltpu.HBM) for v in (coord, *flat)])
    out, cost = pl.pallas_call(
        finish_kernel,
        grid=(ELEM // 128,),
        out_shape=(
            jax.ShapeDtypeStruct((ELEM, NODES), F32),
            jax.ShapeDtypeStruct((1, 1), F32),
        ),
        in_specs=[
            pl.BlockSpec((NODES, 128), lambda i: (0, i)),
            pl.BlockSpec((1, 128), lambda i: (0, 0)),
        ],
        out_specs=(
            pl.BlockSpec((128, NODES), lambda i: (i, 0)),
            pl.BlockSpec(memory_space=pltpu.SMEM),
        ),
        compiler_params=pltpu.CompilerParams(vmem_limit_bytes=16 * 1024 * 1024),
    )(mid, cost_row)
    return out.reshape(4, 8, 8, NODES), cost.reshape(())


def solution(mesh):
    n_grp, n_dev = mesh.shape["grp"], mesh.shape["dev"]
    rows = P(("grp", "dev"))

    def step(obs_coord, obs_resid, obs_weight, obs_dest, obs_send_slot, obs_elem, obs_slot):
        del obs_slot
        return on_device(
            obs_coord, obs_resid, obs_weight, obs_dest, obs_send_slot, obs_elem, n_grp, n_dev
        )

    return jax.shard_map(
        step,
        mesh=mesh,
        in_specs=(P(None, ("grp", "dev")), rows, rows, rows, rows, rows, rows),
        out_specs=(P("grp", "dev", None, None), P()),
        check_vma=False,
    )
```

```python
import functools
import math

import jax
import jax.numpy as jnp
from jax import lax
from jax.experimental import pallas as pl
from jax.experimental.pallas import tpu as pltpu
from jax.sharding import PartitionSpec as P

CAP = 128
ELEM = 256
NODES = 512
COPLANE = 16
PEERS = 64
NODE_POINTS = [-math.cos(math.pi * k / 7) for k in range(8)]
NODE_SCALE = [
    1.0 / math.prod(NODE_POINTS[a] - NODE_POINTS[m] for m in range(8) if m != a)
    for a in range(8)
]
NT = (((1,), (1,)), ((), ()))
F32, BF16, I32 = jnp.float32, jnp.bfloat16, jnp.int32
EDGE = (0, 7)
OUTER = [(a, b) for a in range(8) for b in range(8) if a in EDGE or b in EDGE]
INNER = [(a, b) for a in range(8) for b in range(8) if not (a in EDGE or b in EDGE)]
OUTER.sort(key=lambda ab: (EDGE.index(ab[0]) if ab[0] in EDGE else 2, ab))
GROUPS = OUTER + INNER
PLACE = {ab: 8 * i for i, ab in enumerate(GROUPS)}
SPLIT = 8 * len(OUTER)


def peer_steps(n_dev):
    size_y, size_z = n_dev // min(COPLANE, n_dev), min(COPLANE, n_dev) // 2
    steps = [(y, z, c) for y in range(size_y) for z in range(size_z) for c in range(2)]

    def hops(step):
        y, z, _ = step
        return min(y, size_y - y) + min(z, size_z - z)

    return sorted(steps, key=lambda step: (hops(step), step))


def bounds_of(n_dev):
    return [0, 8, 24, 40, 52, 64] if n_dev == 64 else [0, 2, 4]


def lanes_of(shape):
    return lax.broadcasted_iota(I32, shape, len(shape) - 1)


def rows_of(shape):
    return lax.broadcasted_iota(I32, shape, len(shape) - 2)


def high_of(value):
    return value.astype(BF16).astype(F32)


def one_hot(ids, count):
    shape = (count, ids.shape[1])
    ids = jnp.broadcast_to(ids, (16, ids.shape[1])).astype(BF16)
    ids = jnp.concatenate([ids] * (count // 16), axis=0)
    row = rows_of(shape).astype(F32).astype(BF16)
    return jnp.where(row == ids, jnp.ones(shape, BF16), jnp.zeros(shape, BF16))


def basis(t):
    shape = (8, t.shape[1])
    t = jnp.broadcast_to(t, shape)
    square = t * t
    row = rows_of(shape)
    pair = jnp.minimum(row, 7 - row)
    point, scale = F32(NODE_POINTS[7]), F32(NODE_SCALE[7])
    for a in range(7):
        point = jnp.where(row == a, F32(NODE_POINTS[a]), point)
        scale = jnp.where(row == a, F32(NODE_SCALE[a]), scale)
    own = (t + point) * scale
    out = None
    for m in range(4):
        factor = jnp.where(pair == m, own, square - F32(NODE_POINTS[m] ** 2))
        out = factor if out is None else out * factor
    return out


def move(x, k):
    return pltpu.roll(x, k % x.shape[1], 1)


def exchange_kernel(
    n_grp, n_dev, coord, resid, weight, dest, slot, elem, mid, cost,
    coord_v, resid_v, weight_v, dest_v, slot_v, elem_v,
    lhs, pick, send, recv, acc, outer, summed, bases, xo, xi, oh,
    c1s, c1r, c2s, c2r, halo_g, halo_d, halo_c, gsend, dsend,
    in_sem, send_sem, recv_sem, c1_ssem, c1_rsem, c2_ssem, c2_rsem, h_ssem, h_rsem,
):
    g, d = lax.axis_index("grp"), lax.axis_index("dev")
    co = min(COPLANE, n_dev)
    planes = n_dev // co
    steps = peer_steps(n_dev)
    here = lax.rem(d, co)
    block = d - here
    y, z, core = d // co, here // 2, lax.rem(d, 2)
    to_y = [lax.rem(y + k, planes) * co for k in range(planes)]
    to_z = [lax.rem(z + k, co // 2) * 2 for k in range(co // 2)]
    to_core = [core, 1 - core]
    peer_at = [to_y[i] + to_z[j] + to_core[k] for i, j, k in steps]

    def at(dg, dd):
        return {"grp": lax.rem(g + dg + n_grp, n_grp), "dev": lax.rem(d + dd + n_dev, n_dev)}

    loads = [
        pltpu.make_async_copy(src, dst, in_sem.at[i])
        for i, (src, dst) in enumerate(
            [(dest, dest_v), (slot, slot_v), (elem, elem_v), (coord, coord_v), (resid, resid_v), (weight, weight_v)]
        )
    ]
    barrier = pltpu.get_barrier_semaphore()
    corners = [(-1, -1), (-1, 1), (1, -1), (1, 1)]
    peers = [(k, p * co) for k in range(1, n_grp) for p in range(planes)]
    peers += corners
    targets = [{"grp": g, "dev": peer} for peer in reversed(peer_at[1:])]
    targets += [at(dg, dd) for dg, dd in peers]
    for i, target in enumerate(targets):
        if i == len(targets) // 2:
            for load in loads:
                load.start()
        pl.semaphore_signal(barrier, inc=1, device_id=target)
    for load in loads:
        load.wait()

    for j in range(resid_v.shape[0] // 2):
        def pair(ref):
            return jnp.concatenate([ref[2 * j : 2 * j + 1, :], ref[2 * j + 1 : 2 * j + 2, :]], axis=1)

        cols = slice(256 * j, 256 * j + 256)
        to = pair(dest_v)
        upper = to >> 5
        mask = one_hot((to - 32 * upper).astype(F32), 32)
        pick[:, cols] = one_hot((upper * CAP + pair(slot_v)).astype(F32), 256)
        parts = []
        for value in [coord_v[c : c + 1, cols] for c in range(3)] + [pair(weight_v) * pair(resid_v)]:
            high = high_of(value)
            parts += [high, value - high]
        parts.append(pair(elem_v).astype(F32))
        for i, part in enumerate(parts):
            wide = jnp.broadcast_to(part, (16, 256)).astype(BF16)
            lhs[32 * i : 32 * i + 32, cols] = mask * jnp.concatenate([wide, wide], axis=0)
    packed = lax.dot_general(lhs[...], pick[...], NT, preferred_element_type=F32)
    part = [packed[32 * k : 32 * k + 32] for k in range(9)]
    values = [part[2 * c] + part[2 * c + 1] for c in range(4)] + [part[8]]
    for c, value in enumerate(values):
        send[0:32, c, :] = value[:, :CAP]
        send[32:64, c, :] = value[:, CAP:]
    r = resid_v[...]
    c1s[...] = jnp.sum(weight_v[...] * r * r, axis=0, keepdims=True)

    recv[0] = send[d]
    c1r[here] = c1s[...]

    pl.semaphore_wait(barrier, len(targets))

    bounds = bounds_of(n_dev)
    chunks = list(zip(bounds[:-1], bounds[1:]))
    chunk_of = [i for i, (first, last) in enumerate(chunks) for _ in range(first, last)]

    def message(k):
        to = peer_at[k]
        return pltpu.make_async_remote_copy(
            src_ref=send.at[to],
            dst_ref=recv.at[k],
            send_sem=send_sem,
            recv_sem=recv_sem.at[chunk_of[k]],
            device_id={"grp": g, "dev": to},
        )

    def await_bytes(ref, sem):
        pltpu.make_async_copy(ref, ref, sem).wait()

    def partial_one(k):
        return pltpu.make_async_remote_copy(
            src_ref=c1s, dst_ref=c1r.at[here], send_sem=c1_ssem, recv_sem=c1_rsem,
            device_id={"grp": g, "dev": block + lax.rem(here + k, co)},
        )

    for k in range(1, n_dev):
        message(k).start()
        if k == n_dev // 4:
            for j in range(1, co):
                partial_one(j).start()

    mine = g * planes + block // co
    rest = [(k, p) for k in range(n_grp) for p in range(planes) if k or p]
    twos = [
        pltpu.make_async_remote_copy(
            src_ref=c2s, dst_ref=c2r.at[mine], send_sem=c2_ssem, recv_sem=c2_rsem,
            device_id=at(k, p * co),
        )
        for k, p in rest
    ]

    def rows_built(ref, cols, groups, fa, fb, fc):
        bc = [fb[b : b + 1] * fc for b in range(8)]
        count = 8 * len(groups)
        for k in range(0, len(groups), 2):
            full = jnp.concatenate([fa[a : a + 1] * bc[b] for a, b in groups[k : k + 2]], axis=0)
            high = full.astype(BF16)
            low = (full - high.astype(F32)).astype(BF16)
            ref[8 * k : 8 * k + 16, cols] = high
            ref[count + 8 * k : count + 8 * k + 16, cols] = low

    def cols_of(i, p):
        begin = 256 * p - CAP * chunks[i][0]
        return slice(begin, begin + 256)

    def build(i, p):
        first, second = recv[2 * p], recv[2 * p + 1]

        def row(c):
            return jnp.concatenate([first[c : c + 1], second[c : c + 1]], axis=1)

        cols = cols_of(i, p)
        fa = basis(row(0)) * row(3)
        fb = basis(row(1))
        fc = basis(row(2))
        for c, value in enumerate((fa, fb, fc)):
            bases[c, p] = value
        rows_built(xo[i], cols, OUTER, fa, fb, fc)
        oh[i][:, cols] = one_hot(row(4), ELEM)

    def product(ref, i):
        return lax.dot_general(ref[i][...], oh[i][...], NT, preferred_element_type=F32)

    def arrived(i):
        first, last = max(chunks[i][0], 1), chunks[i][1]
        await_bytes(recv.at[first:last], recv_sem.at[i])

    def block_of(body):
        pl.when(d >= 0)(body)

    def inner_rows(which, total):
        left = None
        for i in which:
            for p in range(chunks[i][0] // 2, chunks[i][1] // 2):
                rows_built(xi[i], cols_of(i, p), INNER, *[bases[c, p] for c in range(3)])
            now = product(xi, i)
            left = now if left is None else left + now
        mid[SPLIT:, :] = total + left[: NODES - SPLIT] + left[NODES - SPLIT :]

    for i in range(len(chunks)):
        arrived(i)

        def contract():
            for p in range(chunks[i][0] // 2, chunks[i][1] // 2):
                build(i, p)
            now = product(xo, i)
            if i > 0:
                now = acc[...] + now
            if i + 1 < len(chunks):
                acc[...] = now
            else:
                outer[...] = now[:SPLIT] + now[SPLIT:]

        if i + 1 < len(chunks):
            block_of(contract)
        else:
            contract()

        if i == 0:
            block_of(lambda: inner_rows([0], 0.0))
        if i == 1:
            await_bytes(c1r.at[1:co], c1_rsem)
            total = c1r[0]
            for k in range(1, co):
                total += c1r[k]
            c2s[...] = total
            c2r[mine] = total
            for m in twos:
                m.start()

    def exists(dg, dd):
        return (g + dg >= 0) & (g + dg < n_grp) & (d + dd >= 0) & (d + dd < n_dev)

    halo_steps = [(-1, 0), (1, 0), (0, -1), (0, 1)] + corners
    halo_slots = [halo_g.at[0], halo_g.at[1], halo_d.at[0], halo_d.at[1]]
    halo_slots += [halo_c.at[i] for i in range(4)]

    def halo(i, src):
        dg, dd = halo_steps[i]

        @pl.when(exists(dg, dd))
        def _():
            pltpu.make_async_remote_copy(
                src_ref=src, dst_ref=halo_slots[i], send_sem=h_ssem.at[i], recv_sem=h_rsem.at[i],
                device_id=at(dg, dd),
            ).start()

    def line(a, b):
        first, half = PLACE[a, b], 128 if a else 0
        return outer.at[first : first + 8, half : half + 128]

    for i, (dg, dd) in enumerate(corners):
        halo(4 + i, line(0 if dg < 0 else 7, 0 if dd < 0 else 7))

    lane = lanes_of((8, ELEM))
    half = lanes_of((8, 128))

    def rg(ref, a, b):
        return ref[PLACE[a, b] : PLACE[a, b] + 8, :]

    def put(ref, a, b, value):
        ref[PLACE[a, b] : PLACE[a, b] + 8, :] = value

    now = {ab: rg(outer, *ab) for ab in OUTER}
    for b in (0, 7, 1, 2, 3, 4, 5, 6):
        low, high = now[0, b], now[7, b]
        now[0, b] = low + jnp.where(lane >= 64, move(high, 64), 0.0)
        now[7, b] = high + jnp.where(lane < 192, move(low, -64), 0.0)
        put(summed, 0, b, now[0, b])
        put(summed, 7, b, now[7, b])
    for side, b, step in ((0, 0, 8), (1, 7, -8)):
        near = ((half >> 3) & 7) == b
        for first in (0, 4):
            packed_planes = None
            for j in range(4):
                plane = now[first + j, b]
                left = jnp.where(near, plane[:, :128], 0.0)
                right = jnp.where(near, plane[:, 128:], 0.0)
                piece = move(left + move(right, step), 2 * step * j)
                packed_planes = piece if j == 0 else packed_planes + piece
            dsend[side, 2 * first : 2 * first + 8, :] = packed_planes
    for side in range(2):
        halo(2 + side, dsend.at[side])
    for b in range(4):
        gsend[0, 8 * b : 8 * b + 8, :] = jnp.where(
            half < 64, rg(outer, 0, b)[:, :128], move(rg(outer, 0, b + 4)[:, :128], 64)
        )
        gsend[1, 8 * b : 8 * b + 8, :] = jnp.where(
            half < 64, move(rg(outer, 7, b)[:, 128:], 64), rg(outer, 7, b + 4)[:, 128:]
        )
    for side in range(2):
        halo(side, gsend.at[side])

    @block_of
    def _():
        inner_rows(range(1, len(chunks)), mid[SPLIT:, :])


    for i, (dg, dd) in enumerate(halo_steps):

        @pl.when(exists(-dg, -dd))
        def _():
            await_bytes(halo_slots[i], h_rsem.at[i])


    up_g, down_g = g > 0, g < n_grp - 1
    up_d, down_d = d > 0, d < n_dev - 1
    ey = (lane >> 3) & 7

    def wide(value):
        return jnp.concatenate([value, value], axis=1)

    planes_now = {(a, b): rg(summed if a in EDGE else outer, a, b) for a, b in OUTER}
    for b in range(8):
        part = slice(8 * (b % 4), 8 * (b % 4) + 8)
        from_low, from_high = halo_g[1, part, :], halo_g[0, part, :]
        if b < 4:
            from_high = move(from_high, 64)
        else:
            from_low = move(from_low, 64)
        planes_now[0, b] += jnp.where((lane < 64) & up_g, wide(from_low), 0.0)
        planes_now[7, b] += jnp.where((lane >= 192) & down_g, wide(from_high), 0.0)
    for a in range(8):
        low, high = planes_now[a, 0], planes_now[a, 7]
        part, shift = slice(8 * (a // 4), 8 * (a // 4) + 8), 16 * (a % 4)
        theirs = halo_d[1, part, :]
        to_low = jnp.concatenate([move(theirs, shift - 56), move(theirs, shift - 48)], axis=1)
        theirs = halo_d[0, part, :]
        to_high = jnp.concatenate([move(theirs, 56 - shift), move(theirs, 48 - shift)], axis=1)
        if a == 0:
            to_low += jnp.where((lane < 8) & up_g, wide(move(halo_c[3], -120)), 0.0)
            to_high += jnp.where((lane >= 56) & (lane < 64) & up_g, wide(move(halo_c[2], -8)), 0.0)
        if a == 7:
            to_low += jnp.where((lane >= 192) & (lane < 200) & down_g, wide(move(halo_c[1], 8)), 0.0)
            to_high += jnp.where((lane >= 248) & down_g, wide(move(halo_c[0], 120)), 0.0)
        new_low = jnp.where(ey > 0, move(high, 8), jnp.where(up_d, to_low, 0.0))
        new_high = jnp.where(ey < 7, move(low, -8), jnp.where(down_d, to_high, 0.0))
        planes_now[a, 0] = low + new_low
        planes_now[a, 7] = high + new_high
    for ab in OUTER:
        put(mid, *ab, planes_now[ab])

    await_bytes(c2r.at[1:], c2_rsem)
    total = c2r[0]
    for k in range(1, n_grp * planes):
        total += c2r[k]
    cost[...] = total
    await_bytes(recv.at[1:], send_sem)
    await_bytes(c1r.at[1:], c1_ssem)
    await_bytes(c2r.at[1:], c2_ssem)
    for i, (dg, dd) in enumerate(halo_steps):

        @pl.when(exists(dg, dd))
        def _():
            await_bytes(halo_slots[i], h_ssem.at[i])


def finish_kernel(mid, cost_row, out, cost):
    shape = (8, 128)
    ez = lanes_of(shape) & 7
    row = rows_of(shape)
    done = {}
    for ab in GROUPS:
        now = mid[PLACE[ab] : PLACE[ab] + 8, :]
        z = jnp.where(row == 7, move(now, 1), move(now, -1))
        to_low = jnp.where((row == 0) & (ez > 0), pltpu.roll(z, 1, 0), 0.0)
        to_high = jnp.where((row == 7) & (ez < 7), pltpu.roll(z, 7, 0), 0.0)
        done[ab] = now + to_low + to_high
    for a in range(0, 8, 2):
        both = jnp.concatenate([done[k, b] for k in (a, a + 1) for b in range(8)], axis=0)
        out[:, 64 * a : 64 * a + 128] = both.T
    cost[0, 0] = 0.5 * jnp.sum(cost_row[...])


def on_device(coord, resid, weight, dest, slot, elem, n_grp, n_dev):
    rows = resid.shape[0] // 128
    flat = [v.reshape(rows, 128) for v in (resid, weight, dest, slot, elem)]
    co = min(COPLANE, n_dev)
    blocks = n_grp * (n_dev // co)
    dma = pltpu.SemaphoreType.DMA
    bounds = bounds_of(n_dev)
    widths = [CAP * (last - first) for first, last in zip(bounds[:-1], bounds[1:])]
    vmem = pl.BlockSpec(memory_space=pltpu.VMEM)
    mid, cost_row = pl.pallas_call(
        functools.partial(exchange_kernel, n_grp, n_dev),
        out_shape=(
            jax.ShapeDtypeStruct((NODES, ELEM), F32),
            jax.ShapeDtypeStruct((1, 128), F32),
        ),
        in_specs=[pl.BlockSpec(memory_space=pltpu.HBM)] * 6,
        out_specs=(vmem, vmem),
        scratch_shapes=[
            pltpu.VMEM(coord.shape, F32),
            pltpu.VMEM((rows, 128), F32),
            pltpu.VMEM((rows, 128), F32),
            pltpu.VMEM((rows, 128), I32),
            pltpu.VMEM((rows, 128), I32),
            pltpu.VMEM((rows, 128), I32),
            pltpu.VMEM((9 * 32, rows * 128), BF16),
            pltpu.VMEM((256, rows * 128), BF16),
            pltpu.VMEM((PEERS, 5, CAP), F32),
            pltpu.VMEM((n_dev, 5, CAP), F32),
            pltpu.VMEM((2 * SPLIT, ELEM), F32),
            pltpu.VMEM((SPLIT, ELEM), F32),
            pltpu.VMEM((128, ELEM), F32),
            pltpu.VMEM((3, n_dev // 2, 8, 256), F32),
            [pltpu.VMEM((2 * SPLIT, n), BF16) for n in widths],
            [pltpu.VMEM((2 * (NODES - SPLIT), n), BF16) for n in widths],
            [pltpu.VMEM((ELEM, n), BF16) for n in widths],
            pltpu.VMEM((1, 128), F32),
            pltpu.VMEM((co, 1, 128), F32),
            pltpu.VMEM((1, 128), F32),
            pltpu.VMEM((blocks, 1, 128), F32),
            pltpu.VMEM((2, 32, 128), F32),
            pltpu.VMEM((2, 16, 128), F32),
            pltpu.VMEM((4, 8, 128), F32),
            pltpu.VMEM((2, 32, 128), F32),
            pltpu.VMEM((2, 16, 128), F32),
            dma((6,)),
            dma,
            dma((len(widths),)),
            dma,
            dma,
            dma,
            dma,
            dma((8,)),
            dma((8,)),
        ],
        compiler_params=pltpu.CompilerParams(
            collective_id=0, has_side_effects=True, vmem_limit_bytes=48 * 1024 * 1024
        ),
    )(*[pltpu.with_memory_space_constraint(v, pltpu.HBM) for v in (coord, *flat)])
    out, cost = pl.pallas_call(
        finish_kernel,
        grid=(ELEM // 128,),
        out_shape=(
            jax.ShapeDtypeStruct((ELEM, NODES), F32),
            jax.ShapeDtypeStruct((1, 1), F32),
        ),
        in_specs=[
            pl.BlockSpec((NODES, 128), lambda i: (0, i)),
            pl.BlockSpec((1, 128), lambda i: (0, 0)),
        ],
        out_specs=(
            pl.BlockSpec((128, NODES), lambda i: (i, 0)),
            pl.BlockSpec(memory_space=pltpu.SMEM),
        ),
        compiler_params=pltpu.CompilerParams(vmem_limit_bytes=16 * 1024 * 1024),
    )(mid, cost_row)
    return out.reshape(4, 8, 8, NODES), cost.reshape(())


def solution(mesh):
    n_grp, n_dev = mesh.shape["grp"], mesh.shape["dev"]
    rows = P(("grp", "dev"))

    def step(obs_coord, obs_resid, obs_weight, obs_dest, obs_send_slot, obs_elem, obs_slot):
        del obs_slot
        return on_device(
            obs_coord, obs_resid, obs_weight, obs_dest, obs_send_slot, obs_elem, n_grp, n_dev
        )

    return jax.shard_map(
        step,
        mesh=mesh,
        in_specs=(P(None, ("grp", "dev")), rows, rows, rows, rows, rows, rows),
        out_specs=(P("grp", "dev", None, None), P()),
        check_vma=False,
    )
```
